32 devices in a mesh: q: 32 (over z, y, x, core).
Axes of the slice: x: 2, y: 2, z: 4, core: 2. Of those that a mesh axis runs over, the one named last changes fastest.
Arguments:
- state_in: float32 [2, 33554432], P(None, 'q')
- unitaries: float32 [2, 25, 2, 2], replicated
- cz_pairs: int32 [12, 2], replicated
Outputs:
- output 1: float32 [2, 33554432], P(None, 'q')
- output 2: float32 [25], replicated
All inputs are finite; a program needn't handle non-finite values.
Results may differ from the reference program's by a relative error of at most 0.001.
Values sent between devices are 32-bit elements.
A program may use at most 1 GiB of HBM per device.

```python
import math
import jax
import jax.numpy as jnp
from jax import lax

QUBITS = 25
NUM_PAIRS = QUBITS // 2
STATE_SIZE = 2 ** QUBITS


def u3_gates(theta_angle, phi_angle, lam_angle):
    cos_half = jnp.cos(0.5 * theta_angle)
    sin_half = jnp.sin(0.5 * theta_angle)
    zero_part = jnp.zeros_like(cos_half)
    real_part = jnp.stack([
        jnp.stack([cos_half, -jnp.cos(lam_angle) * sin_half], axis=-1),
        jnp.stack([jnp.cos(phi_angle) * sin_half, jnp.cos(phi_angle + lam_angle) * cos_half], axis=-1)], axis=-2)
    imag_part = jnp.stack([
        jnp.stack([zero_part, -jnp.sin(lam_angle) * sin_half], axis=-1),
        jnp.stack([jnp.sin(phi_angle) * sin_half, jnp.sin(phi_angle + lam_angle) * cos_half], axis=-1)], axis=-2)
    return jnp.stack([real_part, imag_part])


def product_envelope(zero_weight, env_angle):
    env_re = jnp.ones((1,), jnp.float32)
    env_im = jnp.zeros((1,), jnp.float32)
    for qubit_pos in range(QUBITS):
        amp_zero = jnp.sqrt(2.0 * zero_weight[qubit_pos])
        amp_one = jnp.sqrt(2.0 * (1.0 - zero_weight[qubit_pos]))
        fac_re = jnp.stack([amp_zero, amp_one * jnp.cos(env_angle[qubit_pos])])
        fac_im = jnp.stack([jnp.zeros_like(amp_zero), amp_one * jnp.sin(env_angle[qubit_pos])])
        next_re = (env_re[:, None] * fac_re[None, :] - env_im[:, None] * fac_im[None, :]).reshape(-1)
        next_im = (env_re[:, None] * fac_im[None, :] + env_im[:, None] * fac_re[None, :]).reshape(-1)
        env_re = next_re
        env_im = next_im
    return env_re, env_im


def setup_inputs(seed: int = 0) -> dict:
    root_key = jax.random.key(seed)
    key_amp, key_bias, key_theta, key_phase, key_pairs, key_env = jax.random.split(root_key, 6)
    zero_weight = jax.random.uniform(key_bias, (QUBITS,), jnp.float32, 0.15, 0.85)
    env_angle = jax.random.uniform(key_env, (QUBITS,), jnp.float32, 0.0, 2.0 * math.pi)
    env_re, env_im = product_envelope(zero_weight, env_angle)
    noise = 0.6 * jax.random.normal(key_amp, (2, STATE_SIZE), jnp.float32)
    base_re = 1.0 + noise[0]
    base_im = noise[1]
    amplitudes = jnp.stack([env_re * base_re - env_im * base_im, env_re * base_im + env_im * base_re])
    amplitudes = amplitudes * lax.rsqrt(jnp.mean(jnp.sum(amplitudes * amplitudes, axis=0)))
    theta_angle = jax.random.uniform(key_theta, (QUBITS,), jnp.float32, 0.35 * math.pi, 0.65 * math.pi)
    phase_angle = jax.random.uniform(key_phase, (2, QUBITS), jnp.float32, 0.0, 2.0 * math.pi)
    unitaries = u3_gates(theta_angle, phase_angle[0], phase_angle[1])
    cz_pairs = jax.random.permutation(key_pairs, QUBITS)[: 2 * NUM_PAIRS].reshape(NUM_PAIRS, 2).astype(jnp.int32)
    return {'state_in': amplitudes, 'unitaries': unitaries, 'cz_pairs': cz_pairs}


def mix_pair(first, second, coef_a, coef_b):
    out_re = coef_a[0] * first[0] - coef_a[1] * first[1] + coef_b[0] * second[0] - coef_b[1] * second[1]
    out_im = coef_a[0] * first[1] + coef_a[1] * first[0] + coef_b[0] * second[1] + coef_b[1] * second[0]
    return jnp.stack([out_re, out_im])


def apply_gate(state, bit_pos, gate_mat):
    view = state.reshape(2, 2 ** bit_pos, 2, -1)
    zero_half = view[:, :, 0, :]
    one_half = view[:, :, 1, :]
    new_zero = mix_pair(zero_half, one_half, gate_mat[:, 0, 0], gate_mat[:, 0, 1])
    new_one = mix_pair(zero_half, one_half, gate_mat[:, 1, 0], gate_mat[:, 1, 1])
    return jnp.stack([new_zero, new_one], axis=2).reshape(state.shape)


def pair_signs(flat_index, cz_pairs):
    parity = jnp.zeros_like(flat_index)
    for pair_pos in range(NUM_PAIRS):
        shift_a = QUBITS - 1 - cz_pairs[pair_pos, 0]
        shift_b = QUBITS - 1 - cz_pairs[pair_pos, 1]
        parity = parity ^ ((flat_index >> shift_a) & (flat_index >> shift_b) & 1)
    return (1 - 2 * parity).astype(jnp.float32)


def reference(state_in, unitaries, cz_pairs):
    state = state_in
    for qubit_pos in range(QUBITS):
        state = apply_gate(state, qubit_pos, unitaries[:, qubit_pos])
    flat_index = lax.iota(jnp.int32, STATE_SIZE)
    state = state * pair_signs(flat_index, cz_pairs)[None, :]
    density = state[0] * state[0] + state[1] * state[1]
    halves = [jnp.sum(density.reshape(2 ** qubit_pos, 2, -1), axis=(0, 2)) for qubit_pos in range(QUBITS)]
    z_expect = jnp.stack([bit_sums[0] - bit_sums[1] for bit_sums in halves]) / STATE_SIZE
    return state, z_expect
```

```python
import jax
import jax.numpy as jnp
from jax import lax
from jax.experimental import pallas as pl
from jax.experimental.pallas import tpu as pltpu
from jax.sharding import PartitionSpec as P

MESH = pl.DeviceIdType.MESH
LANES = 128
ROWS = 8192
NG = 16
GR = ROWS // NG
NZ = 32
ZR = ROWS // NZ
BLK = 32
NQ = 25
HIGHEST = lax.Precision.HIGHEST


def loop(count, body, unroll=1):
    def step(i, carry):
        body(i)
        return carry
    lax.fori_loop(0, count, step, 0, unroll=unroll)


def cmac(terms):
    out_re = None
    out_im = None
    for (cr, ci), (xr, xi) in terms:
        re = cr * xr - ci * xi
        im = cr * xi + ci * xr
        out_re = re if out_re is None else out_re + re
        out_im = im if out_im is None else out_im + im
    return out_re, out_im


def cprod(a, b):
    return a[0] * b[0] - a[1] * b[1], a[0] * b[1] + a[1] * b[0]


def kernel(x_hbm, u_ref, cz_ref, o_hbm, z_ref,
           psi, abuf, bo, bf, xb, yb, cb, st, kl, ml, acc, tot, r1, r2,
           in_sem, out_sem, ps, ar, bor, bfr, fs, os_, xs, xr, ys, yr, cs, cr_, s1, g1, s2, g2):
    me = lax.axis_index('q')
    z = me // 8
    sub = me % 8
    b = z // 2
    inner = jnp.logical_or(z == 1, z == 2)
    outer = jnp.logical_not(inner)
    dev_out = sub + 24 * b
    dev_mid = sub + 8 * (3 - z)
    dev_in = sub + 8 * (1 + b)
    dev_mid = jnp.where(inner, dev_mid, dev_in)
    dev_out = jnp.where(inner, dev_out, dev_in)
    dev_x = me + 2 - 4 * ((me // 2) % 2)
    dev_y = me + 4 - 8 * ((me // 4) % 2)
    dev_c = me + 1 - 2 * (me % 2)

    def u(q, i, j):
        return u_ref[0, i, j, q], u_ref[1, i, j, q]

    def gate(q):
        return (u(q, 0, 0), u(q, 0, 1)), (u(q, 1, 0), u(q, 1, 1))

    def apply_pair(g, p0, p1):
        return cmac(((g[0][0], p0), (g[0][1], p1))), cmac(((g[1][0], p0), (g[1][1], p1)))

    def rows(start, size):
        return pl.ds(pl.multiple_of(start, 8), size)

    def load(ref, start, size):
        return ref[0, rows(start, size), :], ref[1, rows(start, size), :]

    def store(ref, start, size, val):
        ref[0, rows(start, size), :] = val[0]
        ref[1, rows(start, size), :] = val[1]

    def zslice(ref, k):
        return ref.at[:, rows(k * ZR, ZR), :]

    def gslice(ref, c):
        return ref.at[:, rows(c * GR, GR), :]

    def remote(src, dst, ss, rs, dev):
        return pltpu.make_async_remote_copy(src_ref=src, dst_ref=dst, send_sem=ss, recv_sem=rs,
                                            device_id=(dev,), device_id_type=MESH)

    def own_copy(k):
        return remote(zslice(psi, k), zslice(bo, k), ps.at[k], bor.at[k], dev_mid)

    def up_copy(k):
        return remote(zslice(psi, k), zslice(abuf, k), ps.at[k], ar.at[k], dev_in)

    def fwd_copy(k):
        return remote(zslice(abuf, k), zslice(bf, k), fs.at[k], bfr.at[k], dev_mid)

    def down_copy(k):
        return remote(zslice(abuf, k), zslice(bo, k), os_.at[k], bor.at[k], dev_out)

    def start_z(k):
        @pl.when(inner)
        def _():
            own_copy(k).start()

        @pl.when(outer)
        def _():
            up_copy(k).start()

    def forward(k):
        @pl.when(inner)
        def _():
            up_copy(k).wait_recv()
            fwd_copy(k).start()

    cd = u(0, b, b)
    co = u(0, b, 1 - b)
    w_own = (cprod(cd, u(1, 1 - b, 1 - b)), cprod(cd, u(1, 1 - b, b)),
             cprod(co, u(1, 1 - b, b)), cprod(co, u(1, 1 - b, 1 - b)))
    w_out = (cprod(cd, u(1, b, 1 - b)), cprod(cd, u(1, b, b)),
             cprod(co, u(1, b, b)), cprod(co, u(1, b, 1 - b)))

    def finish_z(k):
        @pl.when(inner)
        def _():
            own_copy(k).wait_send()
            fwd_copy(k).wait_send()
            own_copy(k).wait_recv()
            fwd_copy(k).wait_recv()

            def body(i):
                s = k * ZR + i * BLK
                vals = (load(psi, s, BLK), load(abuf, s, BLK), load(bo, s, BLK), load(bf, s, BLK))
                own = cmac(tuple(zip(w_own, vals)))
                out = cmac(tuple(zip(w_out, vals)))
                store(abuf, s, BLK, out)
                store(bo, s, BLK, own)
            loop(ZR // BLK, body)
            down_copy(k).start()

        @pl.when(outer)
        def _():
            up_copy(k).wait_send()
            down_copy(k).wait_recv()

    def xchg(state, c, stage):
        if stage == 0:
            return remote(gslice(state, c), gslice(xb, c), xs.at[c], xr.at[c], dev_x)
        if stage == 1:
            return remote(gslice(state, c), gslice(yb, c), ys.at[c], yr.at[c], dev_y)
        return remote(gslice(state, c), gslice(cb, c), cs.at[c], cr_.at[c], dev_c)

    bits = ((me // 2) % 2, (me // 4) % 2, me % 2)
    mix_coef = tuple((u(q, v, v), u(q, v, 1 - v)) for q, v in zip((3, 2, 4), bits))

    def mix(state, c, stage):
        cp = xchg(state, c, stage)
        cp.wait_send()
        cp.wait_recv()
        other = (xb, yb, cb)[stage]
        coef = mix_coef[stage]

        def body(i):
            s = c * GR + i * BLK
            store(state, s, BLK, cmac(((coef[0], load(state, s, BLK)), (coef[1], load(other, s, BLK)))))
        loop(GR // BLK, body, unroll=2)

    g9 = gate(9)
    g10 = gate(10)

    def local_gates(state, c):
        base = c * GR

        def rowgates(i):
            p = [load(state, base + j * 128 + i * 16, 16) for j in range(4)]
            p[0], p[2] = apply_pair(g9, p[0], p[2])
            p[1], p[3] = apply_pair(g9, p[1], p[3])
            p[0], p[1] = apply_pair(g10, p[0], p[1])
            p[2], p[3] = apply_pair(g10, p[2], p[3])
            for j in range(4):
                store(state, base + j * 128 + i * 16, 16, p[j])
        loop(8, rowgates)

        def mats(h):
            s = base + h * 256
            a = load(state, s, 128)
            d = load(state, s + 128, 128)
            packed = jnp.concatenate([jnp.concatenate([a[0], d[0]], axis=1),
                                      jnp.concatenate([a[1], d[1]], axis=1)], axis=0)
            m = jnp.dot(ml[...], packed, precision=HIGHEST, preferred_element_type=jnp.float32)
            packed = jnp.concatenate([jnp.concatenate([m[:128, :128], m[128:, :128]], axis=1),
                                      jnp.concatenate([m[:128, 128:], m[128:, 128:]], axis=1)], axis=0)
            m = jnp.dot(packed, kl[...], precision=HIGHEST, preferred_element_type=jnp.float32)
            store(state, s, 256, (m[:, :128], m[:, 128:]))
        loop(2, mats)

    g678 = (gate(6), gate(7), gate(8))

    def chunk_gates(state, first_row):
        def body(i):
            p = [load(state, first_row + j * GR + i * 8, 8) for j in range(8)]
            for g, step in zip(g678, (4, 2, 1)):
                for j in range(8):
                    if not j & step:
                        p[j], p[j + step] = apply_pair(g, p[j], p[j + step])
            for j in range(8):
                store(state, first_row + j * GR + i * 8, 8, p[j])
        loop(GR // 8, body)

    def in_copy(c, slot):
        return pltpu.make_async_copy(x_hbm.at[pl.ds(pl.multiple_of(c * 2 * GR, 8), 2 * GR), :],
                                     st.at[pl.ds(pl.multiple_of(slot * 2 * GR, 8), 2 * GR), :], in_sem.at[slot])

    g5 = gate(5)
    in_copy(0, 0).start()
    in_copy(8, 1).start()

    def phase0(c):
        slot = 2 * (c % 2)
        nxt = 2 - slot

        @pl.when(c < 7)
        def _():
            in_copy(c + 1, nxt).start()
            in_copy(c + 9, nxt + 1).start()
        in_copy(c, slot).wait()
        in_copy(c + 8, slot + 1).wait()

        def body(i):
            s0 = slot * 2 * GR + i * 2 * BLK
            s1_ = s0 + 2 * GR
            lo = st[pl.ds(s0, BLK, stride=2), :], st[pl.ds(s0 + 1, BLK, stride=2), :]
            hi = st[pl.ds(s1_, BLK, stride=2), :], st[pl.ds(s1_ + 1, BLK, stride=2), :]
            n0, n1 = apply_pair(g5, lo, hi)
            store(psi, c * GR + i * BLK, BLK, n0)
            store(psi, (c + 8) * GR + i * BLK, BLK, n1)
        loop(GR // BLK, body)
        start_z(2 * c)
        start_z(2 * c + 1)
    loop(8, phase0)

    row = lax.broadcasted_iota(jnp.int32, (128, 128), 0)
    col = lax.broadcasted_iota(jnp.int32, (128, 128), 1)

    def kron(first, out_idx, in_idx):
        val = None
        for j in range(7):
            g = gate(first + j)
            ob = ((out_idx >> (6 - j)) & 1) == 1
            ib = ((in_idx >> (6 - j)) & 1) == 1
            f = tuple(jnp.where(ob, jnp.where(ib, g[1][1][r], g[1][0][r]), jnp.where(ib, g[0][1][r], g[0][0][r]))
                      for r in range(2))
            val = f if val is None else cprod(val, f)
        return val
    km = kron(18, col, row)
    kl[0:128, 0:128] = km[0]
    kl[0:128, 128:256] = km[1]
    kl[128:256, 0:128] = -km[1]
    kl[128:256, 128:256] = km[0]
    mm = kron(11, row, col)
    ml[0:128, 0:128] = mm[0]
    ml[0:128, 128:256] = -mm[1]
    ml[128:256, 0:128] = mm[1]
    ml[128:256, 128:256] = mm[0]
    chunk_gates(psi, 8 * GR)

    def phase2(i):
        @pl.when(i < 8)
        def _():
            local_gates(psi, 8 + i)
            xchg(psi, 8 + i, 0).start()
            forward(2 * i)
            forward(2 * i + 1)

        @pl.when(jnp.logical_and(i >= 1, i < 9))
        def _():
            mix(psi, 7 + i, 0)
            xchg(psi, 7 + i, 1).start()

        @pl.when(jnp.logical_and(i >= 2, i < 10))
        def _():
            mix(psi, 6 + i, 1)
            xchg(psi, 6 + i, 2).start()

        @pl.when(i >= 3)
        def _():
            mix(psi, 5 + i, 2)
            start_z(2 * (5 + i))
            start_z(2 * (5 + i) + 1)
    loop(11, phase2)

    def phase3(i):
        @pl.when(i < 8)
        def _():
            forward(16 + 2 * i)
            forward(17 + 2 * i)
            finish_z(2 * i)
            finish_z(2 * i + 1)
            local_gates(bo, i)
            xchg(bo, i, 0).start()

        @pl.when(jnp.logical_and(i >= 1, i < 9))
        def _():
            mix(bo, i - 1, 0)
            xchg(bo, i - 1, 1).start()

        @pl.when(jnp.logical_and(i >= 2, i < 10))
        def _():
            mix(bo, i - 2, 1)
            xchg(bo, i - 2, 2).start()

        @pl.when(i >= 3)
        def _():
            mix(bo, i - 3, 2)
    loop(11, phase3)

    chunk_gates(bo, 0)
    acc[...] = jnp.zeros_like(acc)
    flat = lax.broadcasted_iota(jnp.int32, (BLK, LANES), 0) * LANES + lax.broadcasted_iota(jnp.int32, (BLK, LANES), 1)
    shifts = [(NQ - 1 - cz_ref[0, p], NQ - 1 - cz_ref[1, p]) for p in range(12)]

    def out_copy(k):
        slot = k % 4
        return pltpu.make_async_copy(st.at[pl.ds(pl.multiple_of(slot * 2 * ZR, 8), 2 * ZR), :],
                                     o_hbm.at[pl.ds(pl.multiple_of(k * 2 * ZR, 8), 2 * ZR), :], out_sem.at[slot])

    def emit(k, wait):
        if wait:
            out_copy(k - 4).wait()
        slot = k % 4
        tot[k] = jnp.zeros((8, LANES), jnp.float32)

        def body(i):
            re, im = load(bo, k * ZR + i * BLK, BLK)
            idx = flat + (me * (ROWS * LANES) + (k * ZR + i * BLK) * LANES)
            par = None
            for sa, sb in shifts:
                t = lax.shift_right_logical(idx, sa) & lax.shift_right_logical(idx, sb)
                par = t if par is None else par ^ t
            sign = (1 - 2 * (par & 1)).astype(jnp.float32)
            d = re * re + im * im
            acc[rows(i * BLK, BLK), :] += d
            t8 = d[0:8]
            for j in range(1, BLK // 8):
                t8 = t8 + d[8 * j:8 * j + 8]
            tot[k] += t8
            s = slot * 2 * ZR + i * 2 * BLK
            st[pl.ds(s, BLK, stride=2), :] = re * sign
            st[pl.ds(s + 1, BLK, stride=2), :] = im * sign
        loop(ZR // BLK, body)
        out_copy(k).start()
    loop(4, lambda k: emit(k, False))
    loop(12, lambda k: emit(k + 4, True))

    def phase5(j):
        finish_z(16 + j)
        emit(16 + j, True)
    loop(16, phase5)
    loop(4, lambda k: out_copy(28 + k).wait())

    @pl.when(inner)
    def _():
        loop(NZ, lambda k: down_copy(k).wait_send())

    t8 = tot[0]
    for k in range(1, NZ):
        t8 = t8 + tot[k]

    def signed(count, get, bit):
        val = None
        for v in range(count):
            t = get(v)
            neg = (v >> bit) & 1
            if val is None:
                val = t
            else:
                val = val - t if neg else val + t
        return val
    sl = lax.broadcasted_iota(jnp.int32, (8, LANES), 0)
    ln = lax.broadcasted_iota(jnp.int32, (8, LANES), 1)
    vecs = []
    for q in range(5):
        sgn = (1 - 2 * ((me >> (4 - q)) & 1)).astype(jnp.float32)
        vecs.append(t8 * sgn)
    for q in range(5, 10):
        vecs.append(signed(NZ, lambda v: tot[v], 9 - q))
    for q in range(10, 15):
        vecs.append(signed(ZR // 8, lambda v: acc[8 * v:8 * v + 8, :], 14 - q))
    for q in range(15, 18):
        vecs.append(t8 * (1 - 2 * ((sl >> (17 - q)) & 1)).astype(jnp.float32))
    for q in range(18, 25):
        vecs.append(t8 * (1 - 2 * ((ln >> (24 - q)) & 1)).astype(jnp.float32))
    parts = [jnp.sum(v, axis=0, keepdims=True) for v in vecs]
    parts += [jnp.zeros((1, LANES), jnp.float32)] * (32 - NQ)
    r1[pl.ds(sub, 1)] = jnp.concatenate(parts, axis=0)[None]

    def peer1(r):
        p = sub ^ r
        return p, z * 8 + p

    for r in range(1, 8):
        p, dev = peer1(r)
        remote(r1.at[sub], r1.at[sub], s1.at[p], g1.at[sub], dev).start()
    for r in range(1, 8):
        p, dev = peer1(r)
        remote(r1.at[sub], r1.at[p], s1.at[p], g1.at[p], dev).wait_recv()
    val = r1[0]
    for p in range(1, 8):
        val = val + r1[p]
    r2[pl.ds(z, 1)] = val[None]
    for r in range(1, 4):
        p = z ^ r
        remote(r2.at[z], r2.at[z], s2.at[p], g2.at[z], p * 8 + sub).start()
    for r in range(1, 4):
        p = z ^ r
        remote(r2.at[z], r2.at[p], s2.at[p], g2.at[p], p * 8 + sub).wait_recv()
    val = ((r2[0] + r2[1]) + r2[2]) + r2[3]
    for r in range(1, 8):
        p, dev = peer1(r)
        remote(r1.at[sub], r1.at[sub], s1.at[p], g1.at[sub], dev).wait_send()
    for r in range(1, 4):
        p = z ^ r
        remote(r2.at[z], r2.at[z], s2.at[p], g2.at[z], p * 8 + sub).wait_send()
    wide = jnp.concatenate([val, jnp.zeros((LANES - 32, LANES), jnp.float32)], axis=0)
    zrow = jnp.sum(wide.T, axis=0, keepdims=True) * (1.0 / (ROWS * LANES * 32))
    z_ref[...] = zrow[:, :NQ]


def solution(mesh):
    dma = pltpu.SemaphoreType.DMA
    big = pltpu.VMEM((2, ROWS, LANES), jnp.float32)

    def local_layer(state_local, unitaries, cz_pairs):
        x = state_local.reshape(2, ROWS, LANES).transpose(1, 0, 2).reshape(2 * ROWS, LANES)
        gates = unitaries.transpose(0, 2, 3, 1)
        out, z_exp = pl.pallas_call(
            kernel,
            name="gate_layer",
            out_shape=(jax.ShapeDtypeStruct((2 * ROWS, LANES), jnp.float32),
                       jax.ShapeDtypeStruct((1, NQ), jnp.float32)),
            in_specs=[pl.BlockSpec(memory_space=pl.ANY),
                      pl.BlockSpec(memory_space=pltpu.SMEM),
                      pl.BlockSpec(memory_space=pltpu.SMEM)],
            out_specs=(pl.BlockSpec(memory_space=pl.ANY), pl.BlockSpec(memory_space=pltpu.VMEM)),
            scratch_shapes=[big] * 7 + [
                pltpu.VMEM((4 * 2 * GR, LANES), jnp.float32),
                pltpu.VMEM((256, 256), jnp.float32),
                pltpu.VMEM((256, 256), jnp.float32),
                pltpu.VMEM((ZR, LANES), jnp.float32),
                pltpu.VMEM((NZ, 8, LANES), jnp.float32),
                pltpu.VMEM((8, 32, LANES), jnp.float32),
                pltpu.VMEM((4, 32, LANES), jnp.float32),
                dma((4,)), dma((4,)),
                dma((NZ,)), dma((NZ,)), dma((NZ,)), dma((NZ,)), dma((NZ,)), dma((NZ,)),
                dma((NG,)), dma((NG,)), dma((NG,)), dma((NG,)), dma((NG,)), dma((NG,)),
                dma((8,)), dma((8,)), dma((4,)), dma((4,))],
            compiler_params=pltpu.CompilerParams(has_side_effects=True, vmem_limit_bytes=66_000_000),
        )(x, gates, cz_pairs.transpose(1, 0))
        out = out.reshape(ROWS, 2, LANES).transpose(1, 0, 2).reshape(2, ROWS * LANES)
        return out, z_exp.reshape(NQ)

    return jax.shard_map(local_layer, mesh=mesh, in_specs=(P(None, 'q'), P(), P()),
                         out_specs=(P(None, 'q'), P()), check_vma=False)
```

```python
import jax
import jax.numpy as jnp
from jax import lax
from jax.experimental import pallas as pl
from jax.experimental.pallas import tpu as pltpu
from jax.sharding import PartitionSpec as P

MESH = pl.DeviceIdType.MESH
LANES = 128
ROWS = 8192
NG = 16
GR = ROWS // NG
NF = 8
NS = 32
SR = 128
HALF = ROWS // 2
BLK = 32
NQ = 25
HIGHEST = lax.Precision.HIGHEST
VMEM_LIMIT = 50 * 2 ** 20


def loop(count, body, unroll=1):
    def step(i, carry):
        body(i)
        return carry
    lax.fori_loop(0, count, step, 0, unroll=unroll)


def cmac(terms):
    out_re = None
    out_im = None
    for (cr, ci), (xr, xi) in terms:
        re = cr * xr - ci * xi
        im = cr * xi + ci * xr
        out_re = re if out_re is None else out_re + re
        out_im = im if out_im is None else out_im + im
    return out_re, out_im


def cprod(a, b):
    return a[0] * b[0] - a[1] * b[1], a[0] * b[1] + a[1] * b[0]


def kernel(x_hbm, u_ref, cz_ref, o_ref, z_ref,
           psi, abuf, bo, bf, xb, yb, cb, st, kl, ml, acc, tot, diff, fvec, gvec, msg,
           in_sem, ps, ar, bor, bfr, fs, os_, xs, xr, ys, yr, cs, cr_, vs, vr, ms, mr):
    me = lax.axis_index('q')
    z = me // 8
    sub = me % 8
    b = z // 2
    inner = jnp.logical_or(z == 1, z == 2)
    outer = jnp.logical_not(inner)
    dev_in = sub + 8 * (1 + b)
    dev_mid = jnp.where(inner, sub + 8 * (3 - z), dev_in)
    dev_out = jnp.where(inner, sub + 24 * b, dev_in)
    dev_x = me + 2 - 4 * ((me // 2) % 2)
    dev_y = me + 4 - 8 * ((me // 4) % 2)
    dev_c = me + 1 - 2 * (me % 2)

    def in_copy(c, slot):
        return pltpu.make_async_copy(x_hbm.at[pl.ds(pl.multiple_of(c * 2 * GR, 8), 2 * GR), :],
                                     st.at[pl.ds(pl.multiple_of(slot * 2 * GR, 8), 2 * GR), :], in_sem.at[slot])

    in_copy(0, 0).start()
    in_copy(8, 1).start()

    barrier = pltpu.get_barrier_semaphore()

    def greet(dev):
        pl.semaphore_signal(barrier, inc=1, device_id=(dev,), device_id_type=MESH)

    greet(dev_x)
    greet(dev_y)
    greet(dev_c)
    greet(dev_mid)

    @pl.when(inner)
    def _():
        greet(dev_out)
        pl.semaphore_wait(barrier, 5)

    @pl.when(outer)
    def _():
        pl.semaphore_wait(barrier, 4)

    def u(q, i, j):
        return u_ref[0, i, j, q], u_ref[1, i, j, q]

    def gate(q):
        return (u(q, 0, 0), u(q, 0, 1)), (u(q, 1, 0), u(q, 1, 1))

    def apply_pair(g, p0, p1):
        return cmac(((g[0][0], p0), (g[0][1], p1))), cmac(((g[1][0], p0), (g[1][1], p1)))

    def rows(start, size):
        return pl.ds(pl.multiple_of(start, 8), size)

    def load(ref, start, size):
        return ref[0, rows(start, size), :], ref[1, rows(start, size), :]

    def store(ref, start, size, val):
        ref[0, rows(start, size), :] = val[0]
        ref[1, rows(start, size), :] = val[1]

    def gslice(ref, c):
        return ref.at[:, rows(c * GR, GR), :]

    def remote(src, dst, ss, rs, dev):
        return pltpu.make_async_remote_copy(src_ref=src, dst_ref=dst, send_sem=ss, recv_sem=rs,
                                            device_id=(dev,), device_id_type=MESH)

    def zslice(ref, half, k):
        if half == 0:
            return ref.at[:, rows(k * GR, GR), :]
        return ref.at[:, rows(HALF + k * SR, SR), :]

    def own_copy(half, k):
        n = k + half * NF
        return remote(zslice(psi, half, k), zslice(bo, half, k), ps.at[n], bor.at[n], dev_mid)

    def up_copy(half, k):
        n = k + half * NF
        return remote(zslice(psi, half, k), zslice(abuf, half, k), ps.at[n], ar.at[n], dev_in)

    def fwd_copy(half, k):
        n = k + half * NF
        return remote(zslice(abuf, half, k), zslice(bf, half, k), fs.at[n], bfr.at[n], dev_mid)

    def down_copy(half, k):
        n = k + half * NF
        return remote(zslice(abuf, half, k), zslice(bo, half, k), os_.at[n], bor.at[n], dev_out)

    cd = u(0, b, b)
    co = u(0, b, 1 - b)
    w_own = (cprod(cd, u(1, 1 - b, 1 - b)), cprod(cd, u(1, 1 - b, b)),
             cprod(co, u(1, 1 - b, b)), cprod(co, u(1, 1 - b, 1 - b)))
    w_out = (cprod(cd, u(1, b, 1 - b)), cprod(cd, u(1, b, b)),
             cprod(co, u(1, b, b)), cprod(co, u(1, b, 1 - b)))

    def fold(d):
        t = d[0:8]
        for j in range(1, BLK // 8):
            t = t + d[8 * j:8 * j + 8]
        return t

    def finish_z(half, k):
        @pl.when(inner)
        def _():
            own_copy(half, k).wait_send()
            fwd_copy(half, k).wait_send()
            own_copy(half, k).wait_recv()
            fwd_copy(half, k).wait_recv()
            if half:
                tot[NS + k] = jnp.zeros((8, LANES), jnp.float32)

            def body(i):
                s = (HALF + k * SR if half else k * GR) + i * BLK
                vals = (load(psi, s, BLK), load(abuf, s, BLK), load(bo, s, BLK), load(bf, s, BLK))
                own = cmac(tuple(zip(w_own, vals)))
                out = cmac(tuple(zip(w_out, vals)))
                store(abuf, s, BLK, out)
                store(bo, s, BLK, own)
                if half:
                    d_own = own[0] * own[0] + own[1] * own[1]
                    d_out = out[0] * out[0] + out[1] * out[1]
                    acc[rows(i * BLK, BLK), :] += d_own + d_out
                    tot[NS + k] += fold(d_own + d_out)
                    diff[...] += fold(d_own - d_out)
            loop((SR if half else GR) // BLK, body)
            down_copy(half, k).start()

        @pl.when(outer)
        def _():
            up_copy(half, k).wait_send()
            down_copy(half, k).wait_recv()

    def xchg(state, c, stage):
        buf, ss, rs, dev = ((xb, xs, xr, dev_x), (yb, ys, yr, dev_y), (cb, cs, cr_, dev_c))[stage]
        return remote(gslice(state, c), gslice(buf, c % 8), ss.at[c], rs.at[c], dev)

    bits = ((me // 2) % 2, (me // 4) % 2, me % 2)
    mix_coef = tuple((u(q, v, v), u(q, v, 1 - v)) for q, v in zip((3, 2, 4), bits))

    def mix(state, c, stage):
        cp = xchg(state, c, stage)
        cp.wait_send()
        cp.wait_recv()
        other = (xb, yb, cb)[stage]
        coef = mix_coef[stage]

        def body(i):
            s = c * GR + i * BLK
            t = (c % 8) * GR + i * BLK
            store(state, s, BLK, cmac(((coef[0], load(state, s, BLK)), (coef[1], load(other, t, BLK)))))
        loop(GR // BLK, body, unroll=2)

    g9 = gate(9)
    g10 = gate(10)

    def local_gates(state, c):
        base = c * GR

        def rowgates(i):
            p = [load(state, base + j * 128 + i * 16, 16) for j in range(4)]
            p[0], p[2] = apply_pair(g9, p[0], p[2])
            p[1], p[3] = apply_pair(g9, p[1], p[3])
            p[0], p[1] = apply_pair(g10, p[0], p[1])
            p[2], p[3] = apply_pair(g10, p[2], p[3])
            for j in range(4):
                store(state, base + j * 128 + i * 16, 16, p[j])
        loop(8, rowgates)

        def mats(h):
            s = base + h * 256
            a = load(state, s, 128)
            d = load(state, s + 128, 128)
            packed = jnp.concatenate([jnp.concatenate([a[0], d[0]], axis=1),
                                      jnp.concatenate([a[1], d[1]], axis=1)], axis=0)
            m = jnp.dot(ml[...], packed, precision=HIGHEST, preferred_element_type=jnp.float32)
            packed = jnp.concatenate([jnp.concatenate([m[:128, :128], m[128:, :128]], axis=1),
                                      jnp.concatenate([m[:128, 128:], m[128:, 128:]], axis=1)], axis=0)
            m = jnp.dot(packed, kl[...], precision=HIGHEST, preferred_element_type=jnp.float32)
            store(state, s, 256, (m[:, :128], m[:, 128:]))
        loop(2, mats)

    g678 = (gate(6), gate(7), gate(8))

    def chunk_gates(state, first_row):
        def body(i):
            p = [load(state, first_row + j * GR + i * 8, 8) for j in range(8)]
            for g, step in zip(g678, (4, 2, 1)):
                for j in range(8):
                    if not j & step:
                        p[j], p[j + step] = apply_pair(g, p[j], p[j + step])
            for j in range(8):
                store(state, first_row + j * GR + i * 8, 8, p[j])
        loop(GR // 8, body)

    g5 = gate(5)

    def phase0(c):
        slot = 2 * (c % 2)
        nxt = 2 - slot

        @pl.when(c < 7)
        def _():
            in_copy(c + 1, nxt).start()
            in_copy(c + 9, nxt + 1).start()
        in_copy(c, slot).wait()
        in_copy(c + 8, slot + 1).wait()

        def body(i):
            s0 = slot * 2 * GR + i * 2 * BLK
            s1_ = s0 + 2 * GR
            lo = st[pl.ds(s0, BLK, stride=2), :], st[pl.ds(s0 + 1, BLK, stride=2), :]
            hi = st[pl.ds(s1_, BLK, stride=2), :], st[pl.ds(s1_ + 1, BLK, stride=2), :]
            n0, n1 = apply_pair(g5, lo, hi)
            store(psi, c * GR + i * BLK, BLK, n0)
            store(psi, (c + 8) * GR + i * BLK, BLK, n1)
        loop(GR // BLK, body)

        @pl.when(inner)
        def _():
            own_copy(0, c).start()

        @pl.when(outer)
        def _():
            up_copy(0, c).start()
    loop(8, phase0)

    row = lax.broadcasted_iota(jnp.int32, (128, 128), 0)
    col = lax.broadcasted_iota(jnp.int32, (128, 128), 1)

    def kron(first, out_idx, in_idx):
        val = None
        for j in range(7):
            g = gate(first + j)
            ob = ((out_idx >> (6 - j)) & 1) == 1
            ib = ((in_idx >> (6 - j)) & 1) == 1
            f = tuple(jnp.where(ob, jnp.where(ib, g[1][1][r], g[1][0][r]), jnp.where(ib, g[0][1][r], g[0][0][r]))
                      for r in range(2))
            val = f if val is None else cprod(val, f)
        return val
    km = kron(18, col, row)
    kl[0:128, 0:128] = km[0]
    kl[0:128, 128:256] = km[1]
    kl[128:256, 0:128] = -km[1]
    kl[128:256, 128:256] = km[0]
    mm = kron(11, row, col)
    ml[0:128, 0:128] = mm[0]
    ml[0:128, 128:256] = -mm[1]
    ml[128:256, 0:128] = mm[1]
    ml[128:256, 128:256] = mm[0]
    chunk_gates(psi, HALF)

    def phase2(i):
        @pl.when(i < 8)
        def _():
            local_gates(psi, 8 + i)
            xchg(psi, 8 + i, 0).start()

            @pl.when(inner)
            def _():
                up_copy(0, i).wait_recv()
                fwd_copy(0, i).start()

        @pl.when(jnp.logical_and(i >= 1, i < 9))
        def _():
            mix(psi, 7 + i, 0)
            xchg(psi, 7 + i, 1).start()

        @pl.when(jnp.logical_and(i >= 2, i < 10))
        def _():
            mix(psi, 6 + i, 1)
            xchg(psi, 6 + i, 2).start()

        @pl.when(i >= 3)
        def _():
            mix(psi, 5 + i, 2)

            @pl.when(outer)
            def _():
                for j in range(4):
                    up_copy(1, 4 * (i - 3) + j).start()
    loop(11, phase2)

    def phase3(i):
        @pl.when(i < 8)
        def _():
            @pl.when(inner)
            def _():
                for j in range(4):
                    own_copy(1, 4 * i + j).start()
                    up_copy(1, 4 * i + j).wait_recv()
                    fwd_copy(1, 4 * i + j).start()
            finish_z(0, i)
            local_gates(bo, i)
            xchg(bo, i, 0).start()

        @pl.when(jnp.logical_and(i >= 1, i < 9))
        def _():
            mix(bo, i - 1, 0)
            xchg(bo, i - 1, 1).start()

        @pl.when(jnp.logical_and(i >= 2, i < 10))
        def _():
            mix(bo, i - 2, 1)
            xchg(bo, i - 2, 2).start()

        @pl.when(i >= 3)
        def _():
            mix(bo, i - 3, 2)
    loop(11, phase3)

    chunk_gates(bo, 0)
    flat = lax.broadcasted_iota(jnp.int32, (BLK, LANES), 0) * LANES + lax.broadcasted_iota(jnp.int32, (BLK, LANES), 1)
    shifts = [(NQ - 1 - cz_ref[0, p], NQ - 1 - cz_ref[1, p]) for p in range(12)]

    def emit(half, k):
        if not half:
            tot[k] = jnp.zeros((8, LANES), jnp.float32)

        def body(i):
            s = half * HALF + k * SR + i * BLK
            re, im = load(bo, s, BLK)
            idx = flat + (me * (ROWS * LANES) + s * LANES)
            par = None
            for sa, sb in shifts:
                t = lax.shift_right_logical(idx, sa) & lax.shift_right_logical(idx, sb)
                par = t if par is None else par ^ t
            sign = (1 - 2 * (par & 1)).astype(jnp.float32)
            if not half:
                d = re * re + im * im
                acc[rows(i * BLK, BLK), :] += d
                tot[k] += fold(d)
            o_ref[pl.ds(2 * s, BLK, stride=2), :] = re * sign
            o_ref[pl.ds(2 * s + 1, BLK, stride=2), :] = im * sign
        loop(SR // BLK, body)

    sl = lax.broadcasted_iota(jnp.int32, (8, LANES), 0)
    ln = lax.broadcasted_iota(jnp.int32, (8, LANES), 1)

    def sgn(bit):
        return (1 - 2 * bit).astype(jnp.float32)

    def signed(terms, bit):
        parts = [-t if (v >> bit) & 1 else t for v, t in enumerate(terms)]
        while len(parts) > 1:
            parts = [parts[v] + parts[v + 1] for v in range(0, len(parts), 2)]
        return parts[0]

    def sums(half):
        units = [tot[half * NS + v] for v in range(NS)]
        total = signed([t for t in units], 30)
        wide = [acc[8 * v:8 * v + 8, :] for v in range(SR // 8)]
        vecs = [total * sgn(b)]
        vecs.append(diff[...] * -sgn(b) if half else total * sgn(z % 2))
        vecs += [total * sgn((me // 2 ** (4 - q)) % 2) for q in range(2, 5)]
        vecs.append(-total if half else total)
        vecs += [signed(units, 10 - q) for q in range(6, 11)]
        vecs += [signed(wide, 14 - q) for q in range(11, 15)]
        vecs += [total * sgn((sl >> (17 - q)) & 1) for q in range(15, 18)]
        vecs += [total * sgn((ln >> (24 - q)) & 1) for q in range(18, 25)]
        parts = [jnp.sum(v, axis=0, keepdims=True) for v in vecs]
        return jnp.concatenate(parts + [jnp.zeros((1, LANES), jnp.float32)] * (32 - NQ), axis=0)

    acc[...] = jnp.zeros_like(acc)
    loop(NS, lambda k: emit(0, k))
    fvec[...] = sums(0)
    up_sums = remote(fvec, gvec, vs, vr, dev_in)

    @pl.when(outer)
    def _():
        up_sums.start()

    @pl.when(inner)
    def _():
        up_sums.wait_recv()
        fvec[...] += gvec[...]
        acc[...] = jnp.zeros_like(acc)
        diff[...] = jnp.zeros_like(diff)

    def phase5(j):
        finish_z(1, j)
        emit(1, j)
    loop(NS - 1, phase5)
    finish_z(1, NS - 1)

    mine = b * 8 + sub

    def msg_copy(r):
        return remote(msg.at[mine], msg.at[mine], ms.at[r], mr.at[mine], (me + r) % 32)

    @pl.when(inner)
    def _():
        wide = jnp.concatenate([fvec[...] + sums(1), jnp.zeros((LANES - 32, LANES), jnp.float32)], axis=0)
        msg[pl.ds(mine, 1)] = jnp.sum(wide.T, axis=0, keepdims=True)[None]
        loop(31, lambda r: msg_copy(r + 1).start())
    emit(1, NS - 1)

    @pl.when(inner)
    def _():
        loop(NF, lambda k: down_copy(0, k).wait_send())
        loop(NS, lambda k: down_copy(1, k).wait_send())

    @pl.when(outer)
    def _():
        up_sums.wait_send()

    def receive(t):
        dev = t % 8 + 8 * (1 + t // 8)

        @pl.when(dev != me)
        def _():
            remote(msg.at[t], msg.at[t], ms.at[0], mr.at[t], dev).wait_recv()
    loop(16, receive)
    val = msg[0]
    for t in range(1, 16):
        val = val + msg[t]
    z_ref[...] = (val * (1.0 / (ROWS * LANES * 32)))[:, :NQ]

    @pl.when(inner)
    def _():
        loop(31, lambda r: msg_copy(r + 1).wait_send())


def solution(mesh):
    dma = pltpu.SemaphoreType.DMA
    big = pltpu.VMEM((2, ROWS, LANES), jnp.float32)
    half = pltpu.VMEM((2, HALF, LANES), jnp.float32)

    def local_layer(state_local, unitaries, cz_pairs):
        x = state_local.reshape(2, ROWS, LANES).transpose(1, 0, 2).reshape(2 * ROWS, LANES)
        gates = unitaries.transpose(0, 2, 3, 1)
        out, z_exp = pl.pallas_call(
            kernel,
            name="gate_layer",
            out_shape=(pltpu.VMEM((2 * ROWS, LANES), jnp.float32), pltpu.VMEM((1, NQ), jnp.float32)),
            in_specs=[pl.BlockSpec(memory_space=pl.ANY),
                      pl.BlockSpec(memory_space=pltpu.SMEM),
                      pl.BlockSpec(memory_space=pltpu.SMEM)],
            out_specs=(pl.BlockSpec(memory_space=pltpu.VMEM), pl.BlockSpec(memory_space=pltpu.VMEM)),
            scratch_shapes=[big] * 4 + [half] * 3 + [
                pltpu.VMEM((4 * 2 * GR, LANES), jnp.float32),
                pltpu.VMEM((256, 256), jnp.float32),
                pltpu.VMEM((256, 256), jnp.float32),
                pltpu.VMEM((SR, LANES), jnp.float32),
                pltpu.VMEM((2 * NS, 8, LANES), jnp.float32),
                pltpu.VMEM((8, LANES), jnp.float32),
                pltpu.VMEM((32, LANES), jnp.float32),
                pltpu.VMEM((32, LANES), jnp.float32),
                pltpu.VMEM((16, 1, LANES), jnp.float32),
                dma((4,))] + [dma((NF + NS,))] * 6 + [dma((NG,))] * 6 + [
                dma(()), dma(()), dma((32,)), dma((16,))],
            compiler_params=pltpu.CompilerParams(has_side_effects=True, collective_id=0,
                                                 vmem_limit_bytes=VMEM_LIMIT),
        )(x, gates, cz_pairs.transpose(1, 0))
        out = out.reshape(ROWS, 2, LANES).transpose(1, 0, 2).reshape(2, ROWS * LANES)
        return out, z_exp.reshape(NQ)

    return jax.shard_map(local_layer, mesh=mesh, in_specs=(P(None, 'q'), P(), P()),
                         out_specs=(P(None, 'q'), P()), check_vma=False)
```

```python
import jax
import jax.numpy as jnp
from jax import lax
from jax.experimental import pallas as pl
from jax.experimental.pallas import tpu as pltpu
from jax.sharding import PartitionSpec as P

MESH = pl.DeviceIdType.MESH
LANES = 128
ROWS = 8192
NG = 16
GR = ROWS // NG
NF = 8
NT = 8
TR = GR // NT
SR = 128
NS = 32
HALF = ROWS // 2
BLK = 32
NQ = 25
NW = 8
HIGHEST = lax.Precision.HIGHEST
VMEM_LIMIT = 50 * 2 ** 20


def loop(count, body, unroll=1):
    def step(i, carry):
        body(i)
        return carry
    lax.fori_loop(0, count, step, 0, unroll=unroll)


def cmac(terms):
    out_re = None
    out_im = None
    for (cr, ci), (xr, xi) in terms:
        re = cr * xr - ci * xi
        im = cr * xi + ci * xr
        out_re = re if out_re is None else out_re + re
        out_im = im if out_im is None else out_im + im
    return out_re, out_im


def cprod(a, b):
    return a[0] * b[0] - a[1] * b[1], a[0] * b[1] + a[1] * b[0]


def kernel(x_hbm, u_hbm, cz_hbm, o_ref, z_ref,
           psi, abuf, bo, bf, xb, yb, cb, st, kl, ml, acc, tot, diff, fvec, gvec, msg, sent, u_ref, cz_ref,
           par_sem, in_sem, ps, ar, bor, bfr, fs, os_, xs, xr, ys, yr, cs, cr_, vs, vr, ms, mr):
    me = lax.axis_index('q')
    z = me // 8
    sub = me % 8
    b = z // 2
    inner = jnp.logical_or(z == 1, z == 2)
    outer = jnp.logical_not(inner)
    dev_in = sub + 8 * (1 + b)
    dev_mid = jnp.where(inner, sub + 8 * (3 - z), dev_in)
    dev_out = jnp.where(inner, sub + 24 * b, dev_in)
    dev_x = me + 2 - 4 * ((me // 2) % 2)
    dev_y = me + 4 - 8 * ((me // 4) % 2)
    dev_c = me + 1 - 2 * (me % 2)

    def in_copy(c, slot):
        return pltpu.make_async_copy(x_hbm.at[pl.ds(pl.multiple_of(c * 2 * GR, 8), 2 * GR), :],
                                     st.at[pl.ds(pl.multiple_of(slot * 2 * GR, 8), 2 * GR), :], in_sem.at[slot])

    barrier = pltpu.get_barrier_semaphore()

    def greet(dev):
        pl.semaphore_signal(barrier, inc=1, device_id=(dev,), device_id_type=MESH)

    greet(dev_x)
    greet(dev_y)
    greet(dev_c)
    greet(dev_mid)

    @pl.when(inner)
    def _():
        greet(dev_out)
    u_copy = pltpu.make_async_copy(u_hbm, u_ref, par_sem.at[0])
    cz_copy = pltpu.make_async_copy(cz_hbm, cz_ref, par_sem.at[1])
    u_copy.start()
    in_copy(0, 0).start()
    in_copy(8, 1).start()
    cz_copy.start()
    u_copy.wait()
    cz_copy.wait()

    @pl.when(inner)
    def _():
        pl.semaphore_wait(barrier, 5)

    @pl.when(outer)
    def _():
        pl.semaphore_wait(barrier, 4)

    def u(q, i, j):
        return u_ref[0, i, j, q], u_ref[1, i, j, q]

    def gate(q):
        return (u(q, 0, 0), u(q, 0, 1)), (u(q, 1, 0), u(q, 1, 1))

    def apply_pair(g, p0, p1):
        return cmac(((g[0][0], p0), (g[0][1], p1))), cmac(((g[1][0], p0), (g[1][1], p1)))

    def rows(start, size):
        return pl.ds(pl.multiple_of(start, 8), size)

    def load(ref, start, size):
        return ref[0, rows(start, size), :], ref[1, rows(start, size), :]

    def store(ref, start, size, val):
        ref[0, rows(start, size), :] = val[0]
        ref[1, rows(start, size), :] = val[1]

    def gslice(ref, c):
        return ref.at[:, rows(c * GR, GR), :]

    def remote(src, dst, ss, rs, dev):
        return pltpu.make_async_remote_copy(src_ref=src, dst_ref=dst, send_sem=ss, recv_sem=rs,
                                            device_id=(dev,), device_id_type=MESH)

    def span(kind, k):
        if kind == 2:
            return (NG - 1) * GR + k * TR, TR
        return (kind * 8 + k) * GR, GR

    def zslice(ref, kind, k):
        return ref.at[:, rows(*span(kind, k)), :]

    def index(kind, k):
        return k + (0, 8, 15)[kind]

    def own_copy(kind, k):
        return remote(zslice(psi, kind, k), zslice(bo, kind, k), ps, bor.at[index(kind, k)], dev_mid)

    def up_copy(kind, k):
        return remote(zslice(psi, kind, k), zslice(abuf, kind, k), ps, ar.at[index(kind, k)], dev_in)

    def fwd_copy(kind, k):
        return remote(zslice(abuf, kind, k), zslice(bf, kind, k), fs, bfr.at[index(kind, k)], dev_mid)

    def down_copy(kind, k):
        return remote(zslice(bf, kind, k), zslice(bo, kind, k), os_, bor.at[index(kind, k)], dev_out)

    cd = u(0, b, b)
    co = u(0, b, 1 - b)
    w_own = (cprod(cd, u(1, 1 - b, 1 - b)), cprod(cd, u(1, 1 - b, b)),
             cprod(co, u(1, 1 - b, b)), cprod(co, u(1, 1 - b, 1 - b)))
    w_out = (cprod(cd, u(1, b, 1 - b)), cprod(cd, u(1, b, b)),
             cprod(co, u(1, b, b)), cprod(co, u(1, b, 1 - b)))

    def fold(d):
        t = d[0:8]
        for j in range(1, BLK // 8):
            t = t + d[8 * j:8 * j + 8]
        return t

    def finish_z(kind, k):
        start, size = span(kind, k)

        @pl.when(inner)
        def _():
            own_copy(kind, k).wait_recv()
            fwd_copy(kind, k).wait_recv()

            def body(i):
                s = start + i * BLK
                vals = (load(psi, s, BLK), load(abuf, s, BLK), load(bo, s, BLK), load(bf, s, BLK))
                own = cmac(tuple(zip(w_own, vals)))
                out = cmac(tuple(zip(w_out, vals)))
                store(bf, s, BLK, out)
                store(bo, s, BLK, own)
                if kind:
                    d_own = own[0] * own[0] + own[1] * own[1]
                    d_out = out[0] * out[0] + out[1] * out[1]
                    acc[rows(s % SR, BLK), :] += d_own + d_out
                    tot[s // SR] += fold(d_own + d_out)
                    diff[...] += fold(d_own - d_out)
            loop(size // BLK, body)
            down_copy(kind, k).start()

        @pl.when(outer)
        def _():
            down_copy(kind, k).wait_recv()

    def xchg(state, c, stage):
        buf, ss, rs, dev = ((xb, xs, xr, dev_x), (yb, ys, yr, dev_y), (cb, cs, cr_, dev_c))[stage]
        return remote(gslice(state, c), gslice(buf, c % 8), ss.at[c % 2], rs.at[c % 8], dev)

    bits = ((me // 2) % 2, (me // 4) % 2, me % 2)
    mix_coef = tuple((u(q, v, v), u(q, v, 1 - v)) for q, v in zip((3, 2, 4), bits))

    def mix(state, c, stage):
        cp = xchg(state, c, stage)
        cp.wait_send()
        cp.wait_recv()
        other = (xb, yb, cb)[stage]
        coef = mix_coef[stage]

        def body(i):
            s = c * GR + i * BLK
            t = (c % 8) * GR + i * BLK
            store(state, s, BLK, cmac(((coef[0], load(state, s, BLK)), (coef[1], load(other, t, BLK)))))
        loop(GR // BLK, body, unroll=2)

    g9 = gate(9)
    g10 = gate(10)

    def local_gates(state, c):
        base = c * GR

        def rowgates(i):
            p = [load(state, base + j * 128 + i * 16, 16) for j in range(4)]
            p[0], p[2] = apply_pair(g9, p[0], p[2])
            p[1], p[3] = apply_pair(g9, p[1], p[3])
            p[0], p[1] = apply_pair(g10, p[0], p[1])
            p[2], p[3] = apply_pair(g10, p[2], p[3])
            for j in range(4):
                store(state, base + j * 128 + i * 16, 16, p[j])
        loop(8, rowgates)

        def mats(h):
            s = base + h * 256
            a = load(state, s, 128)
            d = load(state, s + 128, 128)
            packed = jnp.concatenate([jnp.concatenate([a[0], d[0]], axis=1),
                                      jnp.concatenate([a[1], d[1]], axis=1)], axis=0)
            m = jnp.dot(ml[...], packed, precision=HIGHEST, preferred_element_type=jnp.float32)
            packed = jnp.concatenate([jnp.concatenate([m[:128, :128], m[128:, :128]], axis=1),
                                      jnp.concatenate([m[:128, 128:], m[128:, 128:]], axis=1)], axis=0)
            m = jnp.dot(packed, kl[...], precision=HIGHEST, preferred_element_type=jnp.float32)
            store(state, s, 256, (m[:, :128], m[:, 128:]))
        loop(2, mats)

    g678 = (gate(6), gate(7), gate(8))

    def chunk_gates(state, first_row):
        def body(i):
            p = [load(state, first_row + j * GR + i * 8, 8) for j in range(8)]
            for g, step in zip(g678, (4, 2, 1)):
                for j in range(8):
                    if not j & step:
                        p[j], p[j + step] = apply_pair(g, p[j], p[j + step])
            for j in range(8):
                store(state, first_row + j * GR + i * 8, 8, p[j])
        loop(GR // 8, body)

    g5 = gate(5)

    def phase0(c):
        slot = 2 * (c % 2)
        nxt = 2 - slot

        @pl.when(c < 7)
        def _():
            in_copy(c + 1, nxt).start()
            in_copy(c + 9, nxt + 1).start()
        in_copy(c, slot).wait()
        in_copy(c + 8, slot + 1).wait()

        def body(i):
            s0 = slot * 2 * GR + i * 2 * BLK
            s1_ = s0 + 2 * GR
            lo = st[pl.ds(s0, BLK, stride=2), :], st[pl.ds(s0 + 1, BLK, stride=2), :]
            hi = st[pl.ds(s1_, BLK, stride=2), :], st[pl.ds(s1_ + 1, BLK, stride=2), :]
            n0, n1 = apply_pair(g5, lo, hi)
            store(psi, c * GR + i * BLK, BLK, n0)
            store(psi, (c + 8) * GR + i * BLK, BLK, n1)
        loop(GR // BLK, body)

        @pl.when(inner)
        def _():
            own_copy(0, c).start()

        @pl.when(outer)
        def _():
            up_copy(0, c).start()
    loop(8, phase0)

    row = lax.broadcasted_iota(jnp.int32, (128, 128), 0)
    col = lax.broadcasted_iota(jnp.int32, (128, 128), 1)

    def kron(first, out_idx, in_idx):
        val = None
        for j in range(7):
            g = gate(first + j)
            ob = ((out_idx >> (6 - j)) & 1) == 1
            ib = ((in_idx >> (6 - j)) & 1) == 1
            f = tuple(jnp.where(ob, jnp.where(ib, g[1][1][r], g[1][0][r]), jnp.where(ib, g[0][1][r], g[0][0][r]))
                      for r in range(2))
            val = f if val is None else cprod(val, f)
        return val
    km = kron(18, col, row)
    kl[0:128, 0:128] = km[0]
    kl[0:128, 128:256] = km[1]
    kl[128:256, 0:128] = -km[1]
    kl[128:256, 128:256] = km[0]
    mm = kron(11, row, col)
    ml[0:128, 0:128] = mm[0]
    ml[0:128, 128:256] = -mm[1]
    ml[128:256, 0:128] = mm[1]
    ml[128:256, 128:256] = mm[0]
    chunk_gates(psi, HALF)

    def phase2(i):
        @pl.when(i < 8)
        def _():
            local_gates(psi, 8 + i)
            xchg(psi, 8 + i, 0).start()

            @pl.when(inner)
            def _():
                up_copy(0, i).wait_recv()
                fwd_copy(0, i).start()

        @pl.when(jnp.logical_and(i >= 1, i < 9))
        def _():
            mix(psi, 7 + i, 0)
            xchg(psi, 7 + i, 1).start()

        @pl.when(jnp.logical_and(i >= 2, i < 10))
        def _():
            mix(psi, 6 + i, 1)
            xchg(psi, 6 + i, 2).start()

        @pl.when(i >= 3)
        def _():
            mix(psi, 5 + i, 2)

            @pl.when(outer)
            def _():
                up_copy(1, i - 3).start()
    loop(11, phase2)

    def phase3(i):
        @pl.when(i < 8)
        def _():
            @pl.when(inner)
            def _():
                @pl.when(i < 7)
                def _():
                    own_copy(1, i).start()
                    up_copy(1, i).wait_recv()
                    fwd_copy(1, i).start()

                @pl.when(i == 7)
                def _():
                    up_copy(1, 7).wait_recv()
                    for j in range(NT):
                        own_copy(2, j).start()
                        fwd_copy(2, j).start()
            finish_z(0, i)
            local_gates(bo, i)
            xchg(bo, i, 0).start()

        @pl.when(jnp.logical_and(i >= 1, i < 9))
        def _():
            mix(bo, i - 1, 0)
            xchg(bo, i - 1, 1).start()

        @pl.when(jnp.logical_and(i >= 2, i < 10))
        def _():
            mix(bo, i - 2, 1)
            xchg(bo, i - 2, 2).start()

        @pl.when(i >= 3)
        def _():
            mix(bo, i - 3, 2)
    loop(11, phase3)

    chunk_gates(bo, 0)
    flat = lax.broadcasted_iota(jnp.int32, (BLK, LANES), 0) * LANES + lax.broadcasted_iota(jnp.int32, (BLK, LANES), 1)
    shifts = [(NQ - 1 - cz_ref[0, p], NQ - 1 - cz_ref[1, p]) for p in range(12)]

    def emit(kind, k):
        start, size = span(kind, k)

        def body(i):
            s = start + i * BLK
            re, im = load(bo, s, BLK)
            idx = flat + (me * (ROWS * LANES) + s * LANES)
            par = None
            for sa, sb in shifts:
                t = lax.shift_right_logical(idx, sa) & lax.shift_right_logical(idx, sb)
                par = t if par is None else par ^ t
            sign = (1 - 2 * (par & 1)).astype(jnp.float32)
            if not kind:
                d = re * re + im * im
                acc[rows(s % SR, BLK), :] += d
                tot[s // SR] += fold(d)
            o_ref[pl.ds(2 * s, BLK, stride=2), :] = re * sign
            o_ref[pl.ds(2 * s + 1, BLK, stride=2), :] = im * sign
        loop(size // BLK, body)

    sl = lax.broadcasted_iota(jnp.int32, (8, LANES), 0)
    ln = lax.broadcasted_iota(jnp.int32, (8, LANES), 1)

    def sgn(bit):
        return (1 - 2 * bit).astype(jnp.float32)

    def signed(terms, bit):
        parts = [-t if (v >> bit) & 1 else t for v, t in enumerate(terms)]
        while len(parts) > 1:
            parts = [parts[v] + parts[v + 1] for v in range(0, len(parts), 2)]
        return parts[0]

    def sums(half):
        units = [tot[half * NS + v] for v in range(NS)]
        total = signed([t for t in units], 30)
        wide = [acc[8 * v:8 * v + 8, :] for v in range(SR // 8)]
        vecs = [total * sgn(b)]
        vecs.append(diff[...] * -sgn(b) if half else total * sgn(z % 2))
        vecs += [total * sgn((me // 2 ** (4 - q)) % 2) for q in range(2, 5)]
        vecs.append(-total if half else total)
        vecs += [signed(units, 10 - q) for q in range(6, 11)]
        vecs += [signed(wide, 14 - q) for q in range(11, 15)]
        vecs += [total * sgn((sl >> (17 - q)) & 1) for q in range(15, 18)]
        vecs += [total * sgn((ln >> (24 - q)) & 1) for q in range(18, 25)]
        parts = [jnp.sum(v, axis=0, keepdims=True) for v in vecs]
        return jnp.concatenate(parts + [jnp.zeros((1, LANES), jnp.float32)] * (32 - NQ), axis=0)

    acc[...] = jnp.zeros_like(acc)
    tot[...] = jnp.zeros_like(tot)
    loop(8, lambda k: emit(0, k))
    fvec[...] = sums(0)
    up_sums = remote(fvec, gvec, vs, vr, dev_in)

    @pl.when(outer)
    def _():
        up_sums.start()

    @pl.when(inner)
    def _():
        up_sums.wait_recv()
        fvec[...] += gvec[...]
        acc[...] = jnp.zeros_like(acc)
        diff[...] = jnp.zeros_like(diff)

    def phase5(kind, k):
        finish_z(kind, k)
        emit(kind, k)
    loop(7, lambda k: phase5(1, k))
    loop(NT - 1, lambda k: phase5(2, k))
    finish_z(2, NT - 1)

    mine = b * 8 + sub

    def msg_copy(r):
        return remote(msg.at[mine], msg.at[mine], ms, mr.at[mine], (me + r) % 32)

    @pl.when(inner)
    def _():
        wide = jnp.concatenate([fvec[...] + sums(1), jnp.zeros((LANES - 32, LANES), jnp.float32)], axis=0)
        msg[pl.ds(mine, 1)] = jnp.sum(wide.T, axis=0, keepdims=True)[None]
        loop(31, lambda r: msg_copy(r + 1).start())
    emit(2, NT - 1)

    @pl.when(inner)
    def _():
        remote(abuf, bf, fs, vr, dev_mid).wait_send()
        remote(bf, bo, os_, vr, dev_out).wait_send()

    @pl.when(outer)
    def _():
        up_sums.wait_send()
    remote(psi, bo, ps, vr, dev_mid).wait_send()

    def receive(t):
        dev = t % 8 + 8 * (1 + t // 8)

        @pl.when(dev != me)
        def _():
            remote(msg.at[t], msg.at[t], ms, mr.at[t], dev).wait_recv()
    loop(16, receive)
    val = msg[0]
    for t in range(1, 16):
        val = val + msg[t]
    z_ref[...] = (val * (1.0 / (ROWS * LANES * 32)))[:, :NQ]

    @pl.when(inner)
    def _():
        remote(sent, sent, ms, vr, dev_mid).wait_send()


def writer(s_ref, z_ref, o_hbm, zo_ref, sem):
    copies = [pltpu.make_async_copy(s_ref.at[pl.ds(k * 2 * ROWS // NW, 2 * ROWS // NW), :],
                                    o_hbm.at[pl.ds(k * 2 * ROWS // NW, 2 * ROWS // NW), :], sem.at[k]) for k in range(NW)]
    for cp in copies:
        cp.start()
    zo_ref[...] = z_ref[...]
    for cp in copies:
        cp.wait()


def solution(mesh):
    dma = pltpu.SemaphoreType.DMA
    big = pltpu.VMEM((2, ROWS, LANES), jnp.float32)
    half = pltpu.VMEM((2, HALF, LANES), jnp.float32)

    def local_layer(state_local, unitaries, cz_pairs):
        x = state_local.reshape(2, ROWS, LANES).transpose(1, 0, 2).reshape(2 * ROWS, LANES)
        gates = unitaries.transpose(0, 2, 3, 1)
        out, z_exp = pl.pallas_call(
            kernel,
            name="gate_layer",
            out_shape=(pltpu.VMEM((2 * ROWS, LANES), jnp.float32), pltpu.VMEM((1, NQ), jnp.float32)),
            in_specs=[pl.BlockSpec(memory_space=pl.ANY),
                      pl.BlockSpec(memory_space=pl.ANY),
                      pl.BlockSpec(memory_space=pl.ANY)],
            out_specs=(pl.BlockSpec(memory_space=pltpu.VMEM), pl.BlockSpec(memory_space=pltpu.VMEM)),
            scratch_shapes=[big] * 4 + [half] * 3 + [
                pltpu.VMEM((4 * 2 * GR, LANES), jnp.float32),
                pltpu.VMEM((256, 256), jnp.float32),
                pltpu.VMEM((256, 256), jnp.float32),
                pltpu.VMEM((SR, LANES), jnp.float32),
                pltpu.VMEM((2 * NS, 8, LANES), jnp.float32),
                pltpu.VMEM((8, LANES), jnp.float32),
                pltpu.VMEM((32, LANES), jnp.float32),
                pltpu.VMEM((32, LANES), jnp.float32),
                pltpu.VMEM((16, 1, LANES), jnp.float32),
                pltpu.VMEM((31, 1, LANES), jnp.float32),
                pltpu.SMEM((2, 2, 2, NQ), jnp.float32),
                pltpu.SMEM((2, 12), jnp.int32),
                dma((2,)), dma((4,)), dma(()), dma((16,)), dma((15 + NT,)), dma((15 + NT,)), dma(()), dma(())] + [
                dma((2,)), dma((8,))] * 3 + [dma(()), dma(()), dma(()), dma((16,))],
            compiler_params=pltpu.CompilerParams(has_side_effects=True, collective_id=0,
                                                 vmem_limit_bytes=VMEM_LIMIT),
        )(x, gates, cz_pairs.transpose(1, 0))
        out, z_exp = pl.pallas_call(
            writer,
            name="write_result",
            out_shape=(jax.ShapeDtypeStruct((2 * ROWS, LANES), jnp.float32), jax.ShapeDtypeStruct((1, NQ), jnp.float32)),
            in_specs=[pl.BlockSpec(memory_space=pltpu.VMEM), pl.BlockSpec(memory_space=pltpu.VMEM)],
            out_specs=(pl.BlockSpec(memory_space=pl.ANY), pl.BlockSpec(memory_space=pltpu.VMEM)),
            scratch_shapes=[dma((NW,))],
            compiler_params=pltpu.CompilerParams(vmem_limit_bytes=2 ** 20),
        )(out, z_exp)
        out = out.reshape(ROWS, 2, LANES).transpose(1, 0, 2).reshape(2, ROWS * LANES)
        return out, z_exp.reshape(NQ)

    return jax.shard_map(local_layer, mesh=mesh, in_specs=(P(None, 'q'), P(), P()),
                         out_specs=(P(None, 'q'), P()), check_vma=False)
```

```python
import jax
import jax.numpy as jnp
from jax import lax
from jax.experimental import pallas as pl
from jax.experimental.pallas import tpu as pltpu
from jax.sharding import PartitionSpec as P

MESH = pl.DeviceIdType.MESH
LANES = 128
ROWS = 8192
NG = 16
GR = ROWS // NG
NF = 8
NT = 16
TR = GR // NT
SR = 128
NS = 32
HALF = ROWS // 2
BLK = 32
NQ = 25
NW = 8
NX = 4
LO = slice(0, 128)
HI = slice(128, 256)
HIGHEST = lax.Precision.HIGHEST
VMEM_LIMIT = 50 * 2 ** 20


def loop(count, body, unroll=1):
    def step(i, carry):
        body(i)
        return carry
    lax.fori_loop(0, count, step, 0, unroll=unroll)


def cmac(terms):
    out_re = None
    out_im = None
    for (cr, ci), (xr, xi) in terms:
        re = cr * xr - ci * xi
        im = cr * xi + ci * xr
        out_re = re if out_re is None else out_re + re
        out_im = im if out_im is None else out_im + im
    return out_re, out_im


def cprod(a, b):
    return cmac(((a, b),))


def norm2(a):
    re, im = a
    return re * re + im * im


def kernel(x_hbm, u_hbm, cz_hbm, o_ref, z_ref,
           psi, abuf, bo, bf, xb, yb, cb, st, kl, ml, acc, tot, diff, fvec, gvec, msg, sent, u_ref, cz_ref,
           par_sem, in_sem, ps, ar, bor, bfr, fs, os_, xs, xr, ys, yr, cs, cr_, vs, vr, ms, mr):
    me = lax.axis_index('q')
    z = me // 8
    sub = me % 8
    b = z // 2
    inner = jnp.logical_or(z == 1, z == 2)
    outer = jnp.logical_not(inner)
    dev_in = sub + 8 * (1 + b)
    dev_mid = jnp.where(inner, sub + 8 * (3 - z), dev_in)
    dev_out = jnp.where(inner, sub + 24 * b, dev_in)

    def my_bit(k):
        return (me // 2 ** k) % 2

    dev_c, dev_x, dev_y = [me + 2 ** k * (1 - 2 * my_bit(k)) for k in range(3)]

    def in_copy(c, slot):
        return pltpu.make_async_copy(x_hbm.at[pl.ds(pl.multiple_of(c * 2 * GR, 8), 2 * GR), :],
                                     st.at[pl.ds(pl.multiple_of(slot * 2 * GR, 8), 2 * GR), :], in_sem.at[slot])

    barrier = pltpu.get_barrier_semaphore()

    def greet(dev):
        pl.semaphore_signal(barrier, inc=1, device_id=(dev,), device_id_type=MESH)

    greet(dev_x)
    greet(dev_y)
    greet(dev_c)
    greet(dev_mid)

    @pl.when(inner)
    def _():
        greet(dev_out)
    u_copy = pltpu.make_async_copy(u_hbm, u_ref, par_sem.at[0])
    cz_copy = pltpu.make_async_copy(cz_hbm, cz_ref, par_sem.at[1])
    u_copy.start()
    in_copy(0, 0).start()
    in_copy(8, 1).start()
    cz_copy.start()
    u_copy.wait()
    cz_copy.wait()

    def u(q, i, j):
        return u_ref[0, i, j, q], u_ref[1, i, j, q]

    def gate(q):
        return tuple(tuple(u(q, i, j) for j in range(2)) for i in range(2))

    def apply_pair(g, p0, p1):
        return tuple(cmac(tuple(zip(g_row, (p0, p1)))) for g_row in g)

    def rows(start, size):
        return pl.ds(pl.multiple_of(start, 8), size)

    def load(ref, start, size):
        return ref[0, rows(start, size), :], ref[1, rows(start, size), :]

    def store(ref, start, size, val):
        ref[0, rows(start, size), :] = val[0]
        ref[1, rows(start, size), :] = val[1]

    def gslice(ref, c):
        return ref.at[:, rows(c * GR, GR), :]

    def remote(src, dst, ss, rs, dev):
        return pltpu.make_async_remote_copy(src_ref=src, dst_ref=dst, send_sem=ss, recv_sem=rs,
                                            device_id=(dev,), device_id_type=MESH)

    def span(kind, k):
        if kind == 2:
            return (NG - 1) * GR + k * TR, TR
        return (kind * 8 + k) * GR, GR

    def zslice(ref, kind, k):
        return ref.at[:, rows(*span(kind, k)), :]

    def index(kind, k):
        return k + (0, 8, 15)[kind]

    def own_copy(kind, k):
        return remote(zslice(psi, kind, k), zslice(bo, kind, k), ps, bor.at[index(kind, k)], dev_mid)

    def up_copy(kind, k):
        return remote(zslice(psi, kind, k), zslice(abuf, kind, k), ps, ar.at[index(kind, k)], dev_in)

    def fwd_copy(kind, k):
        return remote(zslice(abuf, kind, k), zslice(bf, kind, k), fs, bfr.at[index(kind, k)], dev_mid)

    def down_copy(kind, k):
        return remote(zslice(bf, kind, k), zslice(bo, kind, k), os_, bor.at[index(kind, k)], dev_out)

    def z_row(hi, lo):
        return [cprod(u(0, hi, v), u(1, lo, w)) for v, w in ((b, 1 - b), (b, b), (1 - b, b), (1 - b, 1 - b))]
    w_own = z_row(b, 1 - b)
    w_out = z_row(b, b)
    w_mid = z_row(1 - b, b)
    w_far = z_row(1 - b, 1 - b)

    def fold(d):
        t = d[0:8]
        for j in range(1, BLK // 8):
            t = t + d[8 * j:8 * j + 8]
        return t

    def finish_z(kind, k, count=2):
        start, size = span(kind, k)

        @pl.when(inner)
        def _():
            own_copy(kind, k).wait_recv()
            fwd_copy(kind, k).wait_recv()

            def body(i):
                s = start + i * BLK
                vals = (load(psi, s, BLK), load(abuf, s, BLK), load(bo, s, BLK), load(bf, s, BLK))
                own = cmac(tuple(zip(w_own, vals)))
                out = cmac(tuple(zip(w_out, vals)))
                store(bf, s, BLK, out)
                store(bo, s, BLK, own)
                if kind and count:
                    d_own = norm2(own)
                    d_out = norm2(out)
                    near = d_own + d_out
                    d0, d1 = near, d_own - d_out
                    if count == 4:
                        d_mid = norm2(cmac(tuple(zip(w_mid, vals))))
                        d_far = norm2(cmac(tuple(zip(w_far, vals))))
                        d0, d1 = near - (d_mid + d_far), d1 + (d_far - d_mid)
                        near = near + (d_mid + d_far)
                    acc[rows(s % SR, BLK), :] += near
                    tot[s // SR] += fold(near)
                    diff[0] += fold(d0)
                    diff[1] += fold(d1)
            loop(size // BLK, body)
            down_copy(kind, k).start()

        @pl.when(outer)
        def _():
            down_copy(kind, k).wait_recv()

    def xchg(state, c, stage):
        buf, ss, rs, dev = ((xb, xs, xr, dev_x), (yb, ys, yr, dev_y), (cb, cs, cr_, dev_c))[stage]
        return remote(gslice(state, c), gslice(buf, c % NX), ss.at[c % 2], rs.at[c % NX], dev)

    bits = [my_bit(k) for k in (1, 2, 0)]
    mix_coef = tuple((u(q, v, v), u(q, v, 1 - v)) for q, v in zip((3, 2, 4), bits))

    def mix(state, c, stage):
        cp = xchg(state, c, stage)
        cp.wait_send()
        cp.wait_recv()
        other = (xb, yb, cb)[stage]
        coef = mix_coef[stage]

        def body(i):
            s = c * GR + i * BLK
            t = (c % NX) * GR + i * BLK
            store(state, s, BLK, cmac(((coef[0], load(state, s, BLK)), (coef[1], load(other, t, BLK)))))
        loop(GR // BLK, body, unroll=2)

    g9 = gate(9)
    g10 = gate(10)

    def local_gates(state, c):
        base = c * GR

        def rowgates(i):
            p = [load(state, base + j * 128 + i * 16, 16) for j in range(4)]
            for g, step in ((g9, 2), (g10, 1)):
                for j in range(4):
                    if not j & step:
                        p[j], p[j + step] = apply_pair(g, p[j], p[j + step])
            for j in range(4):
                store(state, base + j * 128 + i * 16, 16, p[j])
        loop(8, rowgates)

        def mats(h):
            s = base + h * 256
            a = load(state, s, 128)
            d = load(state, s + 128, 128)
            packed = jnp.concatenate([jnp.concatenate(pair, axis=1) for pair in zip(a, d)], axis=0)
            m = jnp.dot(ml[...], packed, precision=HIGHEST, preferred_element_type=jnp.float32)
            packed = jnp.concatenate([jnp.concatenate([m[LO, h], m[HI, h]], axis=1) for h in (LO, HI)], axis=0)
            m = jnp.dot(packed, kl[...], precision=HIGHEST, preferred_element_type=jnp.float32)
            store(state, s, 256, (m[:, LO], m[:, HI]))
        loop(2, mats)

    g678 = (gate(6), gate(7), gate(8))

    def chunk_gates(state, first_row):
        def body(i):
            p = [load(state, first_row + j * GR + i * 8, 8) for j in range(8)]
            for g, step in zip(g678, (4, 2, 1)):
                for j in range(8):
                    if not j & step:
                        p[j], p[j + step] = apply_pair(g, p[j], p[j + step])
            for j in range(8):
                store(state, first_row + j * GR + i * 8, 8, p[j])
        loop(GR // 8, body)

    g5 = gate(5)

    def phase0(c):
        slot = 2 * (c % 2)
        nxt = 2 - slot

        @pl.when(c < 7)
        def _():
            in_copy(c + 1, nxt).start()
            in_copy(c + 9, nxt + 1).start()
        in_copy(c, slot).wait()
        in_copy(c + 8, slot + 1).wait()

        def body(i):
            s0 = slot * 2 * GR + i * 2 * BLK
            s1_ = s0 + 2 * GR
            lo = st[pl.ds(s0, BLK, stride=2), :], st[pl.ds(s0 + 1, BLK, stride=2), :]
            hi = st[pl.ds(s1_, BLK, stride=2), :], st[pl.ds(s1_ + 1, BLK, stride=2), :]
            n0, n1 = apply_pair(g5, lo, hi)
            store(psi, c * GR + i * BLK, BLK, n0)
            store(psi, (c + 8) * GR + i * BLK, BLK, n1)
        loop(GR // BLK, body)

        @pl.when(jnp.logical_and(inner, c == 0))
        def _():
            pl.semaphore_wait(barrier, 5)

        @pl.when(jnp.logical_and(outer, c == 0))
        def _():
            pl.semaphore_wait(barrier, 4)

        @pl.when(inner)
        def _():
            own_copy(0, c).start()

        @pl.when(outer)
        def _():
            up_copy(0, c).start()
    loop(8, phase0)

    row = lax.broadcasted_iota(jnp.int32, (128, 128), 0)
    col = lax.broadcasted_iota(jnp.int32, (128, 128), 1)

    def kron(first, out_idx, in_idx):
        val = None
        for j in range(7):
            g = gate(first + j)
            ob = ((out_idx >> (6 - j)) & 1) == 1
            ib = ((in_idx >> (6 - j)) & 1) == 1
            f = tuple(jnp.where(ob, jnp.where(ib, g[1][1][r], g[1][0][r]), jnp.where(ib, g[0][1][r], g[0][0][r]))
                      for r in range(2))
            val = f if val is None else cprod(val, f)
        return val
    km = kron(18, col, row)
    kl[LO, LO] = km[0]
    kl[LO, HI] = km[1]
    kl[HI, LO] = -km[1]
    kl[HI, HI] = km[0]
    mm = kron(11, row, col)
    ml[LO, LO] = mm[0]
    ml[LO, HI] = -mm[1]
    ml[HI, LO] = mm[1]
    ml[HI, HI] = mm[0]
    chunk_gates(psi, HALF)

    def phase2(i):
        @pl.when(i < 8)
        def _():
            local_gates(psi, 8 + i)
            xchg(psi, 8 + i, 0).start()

            @pl.when(inner)
            def _():
                up_copy(0, i).wait_recv()
                fwd_copy(0, i).start()

        @pl.when(jnp.logical_and(i >= 1, i < 9))
        def _():
            mix(psi, 7 + i, 0)
            xchg(psi, 7 + i, 1).start()

        @pl.when(jnp.logical_and(i >= 2, i < 10))
        def _():
            mix(psi, 6 + i, 1)
            xchg(psi, 6 + i, 2).start()

        @pl.when(i >= 3)
        def _():
            mix(psi, 5 + i, 2)

            @pl.when(outer)
            def _():
                up_copy(1, i - 3).start()
    loop(11, phase2)

    def phase3(i):
        @pl.when(i < 8)
        def _():
            @pl.when(inner)
            def _():
                @pl.when(i < 7)
                def _():
                    own_copy(1, i).start()
                    up_copy(1, i).wait_recv()
                    fwd_copy(1, i).start()

                @pl.when(i == 7)
                def _():
                    up_copy(1, 7).wait_recv()
                    def pieces(t):
                        p = (t + b * (NT // 2)) % NT
                        own_copy(2, p).start()
                        fwd_copy(2, p).start()
                    loop(NT, pieces)
            finish_z(0, i)
            local_gates(bo, i)
            xchg(bo, i, 0).start()

        @pl.when(jnp.logical_and(i >= 1, i < 9))
        def _():
            mix(bo, i - 1, 0)
            xchg(bo, i - 1, 1).start()

        @pl.when(jnp.logical_and(i >= 2, i < 10))
        def _():
            mix(bo, i - 2, 1)
            xchg(bo, i - 2, 2).start()

        @pl.when(i >= 3)
        def _():
            mix(bo, i - 3, 2)
    loop(11, phase3)

    chunk_gates(bo, 0)
    flat = lax.broadcasted_iota(jnp.int32, (BLK, LANES), 0) * LANES + lax.broadcasted_iota(jnp.int32, (BLK, LANES), 1)
    shifts = [(NQ - 1 - cz_ref[0, p], NQ - 1 - cz_ref[1, p]) for p in range(12)]

    def emit(kind, k):
        start, size = span(kind, k)

        def body(i):
            s = start + i * BLK
            re, im = load(bo, s, BLK)
            idx = flat + (me * (ROWS * LANES) + s * LANES)
            par = None
            for sa, sb in shifts:
                t = lax.shift_right_logical(idx, sa) & lax.shift_right_logical(idx, sb)
                par = t if par is None else par ^ t
            sign = (1 - 2 * (par & 1)).astype(jnp.float32)
            if not kind:
                d = norm2((re, im))
                acc[rows(s % SR, BLK), :] += d
                tot[s // SR] += fold(d)
            o_ref[pl.ds(2 * s, BLK, stride=2), :] = re * sign
            o_ref[pl.ds(2 * s + 1, BLK, stride=2), :] = im * sign
        loop(size // BLK, body)

    sl = lax.broadcasted_iota(jnp.int32, (8, LANES), 0)
    ln = lax.broadcasted_iota(jnp.int32, (8, LANES), 1)

    def sgn(bit):
        return (1 - 2 * bit).astype(jnp.float32)

    def signed(terms, bit):
        parts = [-t if (v >> bit) & 1 else t for v, t in enumerate(terms)]
        while len(parts) > 1:
            parts = [parts[v] + parts[v + 1] for v in range(0, len(parts), 2)]
        return parts[0]

    def sums(half):
        units = [tot[half * NS + v] for v in range(NS)]
        total = signed([t for t in units], 30)
        wide = [acc[8 * v:8 * v + 8, :] for v in range(SR // 8)]
        vecs = [diff[0] * sgn(b), diff[1] * -sgn(b)] if half else [total * sgn(b), total * sgn(z % 2)]
        vecs += [total * sgn(my_bit(4 - q)) for q in range(2, 5)]
        vecs.append(-total if half else total)
        vecs += [signed(units, 10 - q) for q in range(6, 11)]
        vecs += [signed(wide, 14 - q) for q in range(11, 15)]
        vecs += [total * sgn((sl >> (17 - q)) & 1) for q in range(15, 18)]
        vecs += [total * sgn((ln >> (24 - q)) & 1) for q in range(18, 25)]
        parts = [jnp.sum(v, axis=0, keepdims=True) for v in vecs]
        return jnp.concatenate(parts + [jnp.zeros((1, LANES), jnp.float32)] * (32 - NQ), axis=0)

    acc[...] = jnp.zeros_like(acc)
    tot[...] = jnp.zeros_like(tot)
    loop(8, lambda k: emit(0, k))
    fvec[...] = sums(0)
    up_sums = remote(fvec, gvec, vs, vr, dev_in)

    @pl.when(outer)
    def _():
        up_sums.start()

    @pl.when(inner)
    def _():
        up_sums.wait_recv()
        fvec[...] += gvec[...]
        acc[...] = jnp.zeros_like(acc)
        diff[...] = jnp.zeros_like(diff)

    def phase5(k):
        finish_z(1, k)
        emit(1, k)
    loop(7, phase5)

    def tail(t, count):
        p = (t + (1 - b) * (NT // 2)) % NT
        finish_z(2, p, count)
        emit(2, p)
    loop(NT // 2, lambda t: tail(t, 4))

    mine = b * 8 + sub

    def msg_copy(r):
        return remote(msg.at[mine], msg.at[mine], ms, mr.at[mine], (me + r) % 32)

    @pl.when(inner)
    def _():
        wide = jnp.concatenate([fvec[...] + sums(1), jnp.zeros((LANES - 32, LANES), jnp.float32)], axis=0)
        msg[pl.ds(mine, 1)] = jnp.sum(wide.T, axis=0, keepdims=True)[None]
        loop(31, lambda r: msg_copy(r + 1).start())

    loop(NT // 2, lambda t: tail(t + NT // 2, 0))

    def receive(t):
        dev = t % 8 + 8 * (1 + t // 8)

        @pl.when(dev != me)
        def _():
            remote(msg.at[t], msg.at[t], ms, mr.at[t], dev).wait_recv()
    loop(16, receive)
    val = msg[0]
    for t in range(1, 16):
        val = val + msg[t]
    z_ref[...] = (val * (1.0 / (ROWS * LANES * 32)))[:, :NQ]

    @pl.when(inner)
    def _():
        remote(abuf, bf, fs, vr, dev_mid).wait_send()
        remote(sent, sent, ms, vr, dev_mid).wait_send()
        remote(bf, bo, os_, vr, dev_out).wait_send()

    @pl.when(outer)
    def _():
        up_sums.wait_send()
    remote(psi, bo, ps, vr, dev_mid).wait_send()


def writer(s_ref, z_ref, o_hbm, zo_ref, sem):
    copies = [pltpu.make_async_copy(s_ref.at[pl.ds(k * 2 * ROWS // NW, 2 * ROWS // NW), :],
                                    o_hbm.at[pl.ds(k * 2 * ROWS // NW, 2 * ROWS // NW), :], sem.at[k]) for k in range(NW)]
    copies.append(pltpu.make_async_copy(z_ref, zo_ref, sem.at[NW]))
    for cp in copies:
        cp.start()
    for cp in copies:
        cp.wait()


def solution(mesh):
    dma = pltpu.SemaphoreType.DMA
    big = pltpu.VMEM((2, ROWS, LANES), jnp.float32)
    slots = pltpu.VMEM((2, NX * GR, LANES), jnp.float32)

    def local_layer(state_local, unitaries, cz_pairs):
        x = state_local.reshape(2, ROWS, LANES).transpose(1, 0, 2).reshape(2 * ROWS, LANES)
        gates = unitaries.transpose(0, 2, 3, 1)
        out, z_exp = pl.pallas_call(
            kernel,
            name="gate_layer",
            out_shape=(pltpu.VMEM((2 * ROWS, LANES), jnp.float32), pltpu.VMEM((1, NQ), jnp.float32)),
            in_specs=[pl.BlockSpec(memory_space=pl.ANY),
                      pl.BlockSpec(memory_space=pl.ANY),
                      pl.BlockSpec(memory_space=pl.ANY)],
            out_specs=(pl.BlockSpec(memory_space=pltpu.VMEM), pl.BlockSpec(memory_space=pltpu.VMEM)),
            scratch_shapes=[big] * 4 + [slots] * 3 + [
                pltpu.VMEM((4 * 2 * GR, LANES), jnp.float32),
                pltpu.VMEM((256, 256), jnp.float32),
                pltpu.VMEM((256, 256), jnp.float32),
                pltpu.VMEM((SR, LANES), jnp.float32),
                pltpu.VMEM((2 * NS, 8, LANES), jnp.float32),
                pltpu.VMEM((2, 8, LANES), jnp.float32),
                pltpu.VMEM((32, LANES), jnp.float32),
                pltpu.VMEM((32, LANES), jnp.float32),
                pltpu.VMEM((16, 1, LANES), jnp.float32),
                pltpu.VMEM((31, 1, LANES), jnp.float32),
                pltpu.SMEM((2, 2, 2, NQ), jnp.float32),
                pltpu.SMEM((2, 12), jnp.int32),
                dma((2,)), dma((4,)), dma(()), dma((16,)), dma((15 + NT,)), dma((15 + NT,)), dma(()), dma(())] + [
                dma((2,)), dma((NX,))] * 3 + [dma(()), dma(()), dma(()), dma((16,))],
            compiler_params=pltpu.CompilerParams(has_side_effects=True, collective_id=0,
                                                 vmem_limit_bytes=VMEM_LIMIT),
        )(x, gates, cz_pairs.transpose(1, 0))
        out, z_exp = pl.pallas_call(
            writer,
            name="write_result",
            out_shape=(jax.ShapeDtypeStruct((2 * ROWS, LANES), jnp.float32), jax.ShapeDtypeStruct((1, NQ), jnp.float32)),
            in_specs=[pl.BlockSpec(memory_space=pltpu.VMEM), pl.BlockSpec(memory_space=pltpu.VMEM)],
            out_specs=(pl.BlockSpec(memory_space=pl.ANY), pl.BlockSpec(memory_space=pl.ANY)),
            scratch_shapes=[dma((NW + 1,))],
            compiler_params=pltpu.CompilerParams(vmem_limit_bytes=2 ** 20),
        )(out, z_exp)
        out = out.reshape(ROWS, 2, LANES).transpose(1, 0, 2).reshape(2, ROWS * LANES)
        return out, z_exp.reshape(NQ)

    return jax.shard_map(local_layer, mesh=mesh, in_specs=(P(None, 'q'), P(), P()),
                         out_specs=(P(None, 'q'), P()), check_vma=False)
```

```python
import jax
import jax.numpy as jnp
from jax import lax
from jax.experimental import pallas as pl
from jax.experimental.pallas import tpu as pltpu
from jax.sharding import PartitionSpec as P

MESH = pl.DeviceIdType.MESH
LANES = 128
ROWS = 8192
NG = 16
GR = ROWS // NG
PIECES = (256, 256, 128, 128, 64, 32, 32)
SIDE = GR // 2
DR = 128
DP = 64
NT = len(PIECES)
NZ = NG - 2 + NT
FIRST = 128
SR = 128
NS = 32
HALF = ROWS // 2
BLK = 32
NQ = 25
NW = 8
NX = 4
LO = slice(0, 128)
HI = slice(128, 256)
HIGHEST = lax.Precision.HIGHEST
VMEM_LIMIT = 50 * 2 ** 20


def loop(count, body, unroll=1):
    def step(i, carry):
        body(i)
        return carry
    lax.fori_loop(0, count, step, 0, unroll=unroll)


def cmac(terms):
    out_re = None
    out_im = None
    for (cr, ci), (xr, xi) in terms:
        re = cr * xr - ci * xi
        im = cr * xi + ci * xr
        out_re = re if out_re is None else out_re + re
        out_im = im if out_im is None else out_im + im
    return out_re, out_im


def cprod(a, b):
    return cmac(((a, b),))


def norm2(a):
    re, im = a
    return re * re + im * im


def kernel(x_hbm, u_hbm, cz_hbm, o_ref, z_ref,
           psi, abuf, bo, bf, xb, yb, cb, st, kl, ml, acc, tot, diff, fvec, gvec, msg, sent, pm, pf, rp, u_ref, cz_ref,
           par_sem, in_sem, ps, ar, br, fs, os_, xs, xr, ys, yr, cs, cr_, vs, vr, ms, mr, er, dr):
    me = lax.axis_index('q')
    z = me // 8
    sub = me % 8
    b = z // 2
    inner = jnp.logical_or(z == 1, z == 2)
    outer = jnp.logical_not(inner)
    dev_in = sub + 8 * (1 + b)
    dev_mid = jnp.where(inner, sub + 8 * (3 - z), dev_in)
    dev_out = jnp.where(inner, sub + 24 * b, dev_in)

    def my_bit(k):
        return (me // 2 ** k) % 2

    dev_c, dev_x, dev_y = [me + 2 ** k * (1 - 2 * my_bit(k)) for k in range(3)]

    def in_copy(c, slot, sem, start=0, size=GR):
        return pltpu.make_async_copy(x_hbm.at[pl.ds(pl.multiple_of((c * GR + start) * 2, 8), 2 * size), :],
                                     st.at[pl.ds(pl.multiple_of((slot * GR + start) * 2, 8), 2 * size), :], in_sem.at[sem])

    def in_pair(c, slot, sem, start=0, size=GR):
        return in_copy(c, slot, sem, start, size), in_copy(c + 8, slot + 1, sem + 1, start, size)

    part_a = in_pair(0, 0, 0, 0, FIRST)
    part_b = in_pair(0, 0, 2, FIRST, GR - FIRST)

    barrier = pltpu.get_barrier_semaphore()

    def greet(dev):
        pl.semaphore_signal(barrier, inc=1, device_id=(dev,), device_id_type=MESH)

    greet(dev_x)
    greet(dev_y)
    greet(dev_c)
    greet(dev_mid)

    @pl.when(inner)
    def _():
        greet(dev_out)
    u_copy = pltpu.make_async_copy(u_hbm, u_ref, par_sem.at[0])
    cz_copy = pltpu.make_async_copy(cz_hbm, cz_ref, par_sem.at[1])
    u_copy.start()
    for cp in part_a + part_b:
        cp.start()
    cz_copy.start()
    u_copy.wait()

    def u(q, i, j):
        return u_ref[0, i, j, q], u_ref[1, i, j, q]

    def gate(q):
        return tuple(tuple(u(q, i, j) for j in range(2)) for i in range(2))

    def apply_pair(g, p0, p1):
        return tuple(cmac(tuple(zip(g_row, (p0, p1)))) for g_row in g)

    def rows(start, size):
        return pl.ds(pl.multiple_of(start, 8), size)

    def load(ref, start, size):
        return ref[0, rows(start, size), :], ref[1, rows(start, size), :]

    def store(ref, start, size, val):
        ref[0, rows(start, size), :] = val[0]
        ref[1, rows(start, size), :] = val[1]

    def gslice(ref, c):
        return ref.at[:, rows(c * GR, GR), :]

    def remote(src, dst, ss, rs, dev):
        return pltpu.make_async_remote_copy(src_ref=src, dst_ref=dst, send_sem=ss, recv_sem=rs,
                                            device_id=(dev,), device_id_type=MESH)

    def span(kind, k, hb=0):
        if kind < 2:
            return (kind * 8 + k) * GR, GR
        off = sum(PIECES[:k])
        if off < GR:
            return (NG - 2) * GR + off, PIECES[k]
        side = hb if off < GR + SIDE else 1 - hb
        return (NG - 1) * GR + side * SIDE + off % SIDE, PIECES[k]

    def index(kind, k):
        return k + (0, 8, NG - 2)[kind]

    def zcopy(src, dst, ss, rs, dev, place):
        return remote(src.at[:, rows(*place), :], dst.at[:, rows(*place), :], ss, rs, dev)

    def own_copy(kind, k, place):
        return zcopy(psi, bo, ps, br.at[index(kind, k)], dev_mid, place)

    def up_copy(c, place):
        return zcopy(psi, abuf, ps, ar.at[c], dev_in, place)

    def fwd_copy(kind, k, place):
        return zcopy(abuf, bf, fs, br.at[index(kind, k)], dev_mid, place)

    def down_copy(kind, k, place):
        return zcopy(bf, bo, os_, br.at[index(kind, k)], dev_out, place)

    def direct(hb):
        return NG * GR - hb * SIDE - DR

    early_copy = zcopy(psi, abuf, ps, er, dev_out, (direct(1 - b), DR))
    dev_far = sub + 24 * (1 - b)

    def part(ref, k):
        return ref.at[:, pl.ds(k * DP, DP), :]

    def far_copy(k):
        return remote(part(pf, k), part(rp, k), os_, dr.at[k], dev_far)

    def mid_copy(k):
        return remote(part(pm, k), part(rp, k), fs, dr.at[k], dev_mid)

    def send_both(kind, k, hb=0):
        own_copy(kind, k, span(kind, k, hb)).start()
        fwd_copy(kind, k, span(kind, k, hb)).start()

    g5 = gate(5)

    def gate5(c, slot, start=0, size=GR):
        def body(i):
            r = start + i * BLK
            s0 = (slot * GR + r) * 2
            s1 = s0 + 2 * GR
            lo = st[pl.ds(s0, BLK, stride=2), :], st[pl.ds(s0 + 1, BLK, stride=2), :]
            hi = st[pl.ds(s1, BLK, stride=2), :], st[pl.ds(s1 + 1, BLK, stride=2), :]
            n0, n1 = apply_pair(g5, lo, hi)
            store(psi, c * GR + r, BLK, n0)
            store(psi, (c + 8) * GR + r, BLK, n1)
        loop(size // BLK, body)

    def send_first(c, start=0, size=GR):
        place = (c * GR + start, size)

        @pl.when(inner)
        def _():
            own_copy(0, c, place).start()

        @pl.when(outer)
        def _():
            up_copy(c, place).start()

    for cp in part_a:
        cp.wait()
    gate5(0, 0, 0, FIRST)

    @pl.when(inner)
    def _():
        pl.semaphore_wait(barrier, 5)

    @pl.when(outer)
    def _():
        pl.semaphore_wait(barrier, 4)
    send_first(0, 0, FIRST)
    for cp in part_b:
        cp.wait()
    for cp in in_pair(1, 2, 2):
        cp.start()
    gate5(0, 0, FIRST, GR - FIRST)
    send_first(0, FIRST, GR - FIRST)

    def phase0(m):
        c = m + 1
        slot = 2 * (c % 2)
        nxt = 2 - slot

        @pl.when(c < 7)
        def _():
            for cp in in_pair(c + 1, nxt, nxt):
                cp.start()
        for cp in in_pair(c, slot, slot):
            cp.wait()
        gate5(c, slot)
        send_first(c)
    loop(7, phase0)
    cz_copy.wait()
    def z_row(hi, lo):
        return [cprod(u(0, hi, v), u(1, lo, w)) for v, w in ((b, 1 - b), (b, b), (1 - b, b), (1 - b, 1 - b))]
    w_own = z_row(b, 1 - b)
    w_out = z_row(b, b)
    w_mid = z_row(1 - b, b)
    w_far = z_row(1 - b, 1 - b)

    def fold(d):
        t = d[0:8]
        for j in range(1, d.shape[0] // 8):
            t = t + d[8 * j:8 * j + 8]
        return t

    def finish_z(kind, k, count=2):
        start, size = span(kind, k, 1 - b)
        blk = min(BLK, size)

        @pl.when(inner)
        def _():
            zcopy(psi, bo, ps, br.at[index(kind, k)], dev_mid, (0, 2 * size)).wait_recv()

            def body(i):
                s = start + i * blk
                vals = (load(psi, s, blk), load(abuf, s, blk), load(bo, s, blk), load(bf, s, blk))
                own = cmac(tuple(zip(w_own, vals)))
                out = cmac(tuple(zip(w_out, vals)))
                store(bf, s, blk, out)
                store(bo, s, blk, own)
                if kind and count:
                    d_own = norm2(own)
                    d_out = norm2(out)
                    near = d_own + d_out
                    d0, d1 = near, d_own - d_out
                    if count == 4:
                        d_mid = norm2(cmac(tuple(zip(w_mid, vals))))
                        d_far = norm2(cmac(tuple(zip(w_far, vals))))
                        d0, d1 = near - (d_mid + d_far), d1 + (d_far - d_mid)
                        near = near + (d_mid + d_far)
                    acc[rows(s % SR, blk), :] += near
                    tot[s // SR] += fold(near)
                    diff[0] += fold(d0)
                    diff[1] += fold(d1)
            loop(size // blk, body)
            down_copy(kind, k, (start, size)).start()

        @pl.when(outer)
        def _():
            down_copy(kind, k, (start, size)).wait_recv()

    def xchg(state, c, stage):
        buf, ss, rs, dev = ((xb, xs, xr, dev_x), (yb, ys, yr, dev_y), (cb, cs, cr_, dev_c))[stage]
        return remote(gslice(state, c), gslice(buf, c % NX), ss.at[c % 2], rs.at[c % NX], dev)

    bits = [my_bit(k) for k in (1, 2, 0)]
    mix_coef = tuple((u(q, v, v), u(q, v, 1 - v)) for q, v in zip((3, 2, 4), bits))

    def mix(state, c, stage):
        cp = xchg(state, c, stage)
        cp.wait_send()
        cp.wait_recv()
        other = (xb, yb, cb)[stage]
        coef = mix_coef[stage]

        def body(i):
            s = c * GR + i * BLK
            t = (c % NX) * GR + i * BLK
            store(state, s, BLK, cmac(((coef[0], load(state, s, BLK)), (coef[1], load(other, t, BLK)))))
        loop(GR // BLK, body, unroll=2)

    g9 = gate(9)
    g10 = gate(10)

    def local_gates(state, c):
        base = c * GR

        def rowgates(i):
            p = [load(state, base + j * 128 + i * 16, 16) for j in range(4)]
            for g, step in ((g9, 2), (g10, 1)):
                for j in range(4):
                    if not j & step:
                        p[j], p[j + step] = apply_pair(g, p[j], p[j + step])
            for j in range(4):
                store(state, base + j * 128 + i * 16, 16, p[j])
        loop(8, rowgates)

        def mats(h):
            s = base + h * 256
            a = load(state, s, 128)
            d = load(state, s + 128, 128)
            packed = jnp.concatenate([jnp.concatenate(pair, axis=1) for pair in zip(a, d)], axis=0)
            m = jnp.dot(ml[...], packed, precision=HIGHEST, preferred_element_type=jnp.float32)
            packed = jnp.concatenate([jnp.concatenate([m[LO, h], m[HI, h]], axis=1) for h in (LO, HI)], axis=0)
            m = jnp.dot(packed, kl[...], precision=HIGHEST, preferred_element_type=jnp.float32)
            store(state, s, 256, (m[:, LO], m[:, HI]))
        loop(2, mats)

    g678 = (gate(6), gate(7), gate(8))

    def chunk_gates(state, first_row):
        def body(i):
            p = [load(state, first_row + j * GR + i * 8, 8) for j in range(8)]
            for g, step in zip(g678, (4, 2, 1)):
                for j in range(8):
                    if not j & step:
                        p[j], p[j + step] = apply_pair(g, p[j], p[j + step])
            for j in range(8):
                store(state, first_row + j * GR + i * 8, 8, p[j])
        loop(GR // 8, body)

    row = lax.broadcasted_iota(jnp.int32, (128, 128), 0)
    col = lax.broadcasted_iota(jnp.int32, (128, 128), 1)

    def kron(first, out_idx, in_idx):
        val = None
        for j in range(7):
            g = gate(first + j)
            ob = ((out_idx >> (6 - j)) & 1) == 1
            ib = ((in_idx >> (6 - j)) & 1) == 1
            f = tuple(jnp.where(ob, jnp.where(ib, g[1][1][r], g[1][0][r]), jnp.where(ib, g[0][1][r], g[0][0][r]))
                      for r in range(2))
            val = f if val is None else cprod(val, f)
        return val
    km = kron(18, col, row)
    kl[LO, LO] = km[0]
    kl[LO, HI] = km[1]
    kl[HI, LO] = -km[1]
    kl[HI, HI] = km[0]
    mm = kron(11, row, col)
    ml[LO, LO] = mm[0]
    ml[LO, HI] = -mm[1]
    ml[HI, LO] = mm[1]
    ml[HI, HI] = mm[0]
    chunk_gates(psi, HALF)

    def phase2(i):
        @pl.when(i < 8)
        def _():
            local_gates(psi, 8 + i)
            xchg(psi, 8 + i, 0).start()

            @pl.when(inner)
            def _():
                up_copy(i, span(0, i)).wait_recv()
                fwd_copy(0, i, span(0, i)).start()

        @pl.when(jnp.logical_and(i >= 1, i < 9))
        def _():
            mix(psi, 7 + i, 0)
            xchg(psi, 7 + i, 1).start()

        @pl.when(jnp.logical_and(i >= 2, i < 10))
        def _():
            mix(psi, 6 + i, 1)
            xchg(psi, 6 + i, 2).start()

        @pl.when(i >= 3)
        def _():
            mix(psi, 5 + i, 2)

            @pl.when(outer)
            def _():
                up_copy(5 + i, span(1, i - 3)).start()
    loop(11, phase2)

    def phase3(i):
        @pl.when(i < 8)
        def _():
            @pl.when(inner)
            def _():
                @pl.when(i < 6)
                def _():
                    own_copy(1, i, span(1, i)).start()
                    up_copy(8 + i, span(1, i)).wait_recv()
                    fwd_copy(1, i, span(1, i)).start()

                @pl.when(i == 6)
                def _():
                    up_copy(8 + i, span(1, i)).wait_recv()
                    for k in (0, 1):
                        send_both(2, k, b)

                @pl.when(i == 7)
                def _():
                    up_copy(8 + i, span(1, i)).wait_recv()
                    for k in (2, 3, 4):
                        send_both(2, k, b)
                    early_copy.start()
            finish_z(0, i)
            local_gates(bo, i)
            xchg(bo, i, 0).start()

        @pl.when(jnp.logical_and(i >= 1, i < 9))
        def _():
            mix(bo, i - 1, 0)
            xchg(bo, i - 1, 1).start()

        @pl.when(jnp.logical_and(i >= 2, i < 10))
        def _():
            mix(bo, i - 2, 1)
            xchg(bo, i - 2, 2).start()

        @pl.when(i >= 3)
        def _():
            mix(bo, i - 3, 2)
    loop(11, phase3)

    chunk_gates(bo, 0)
    flat = lax.broadcasted_iota(jnp.int32, (BLK, LANES), 0) * LANES + lax.broadcasted_iota(jnp.int32, (BLK, LANES), 1)
    shifts = [(NQ - 1 - cz_ref[0, p], NQ - 1 - cz_ref[1, p]) for p in range(12)]

    def put(s, re, im, blk):
        idx = flat[:blk] + (me * (ROWS * LANES) + s * LANES)
        par = None
        for sa, sb in shifts:
            t = lax.shift_right_logical(idx, sa) & lax.shift_right_logical(idx, sb)
            par = t if par is None else par ^ t
        sign = (1 - 2 * (par & 1)).astype(jnp.float32)
        o_ref[pl.ds(2 * s, blk, stride=2), :] = re * sign
        o_ref[pl.ds(2 * s + 1, blk, stride=2), :] = im * sign

    def emit(kind, k):
        start, size = span(kind, k, 1 - b)
        blk = min(BLK, size)

        def body(i):
            s = start + i * blk
            re, im = load(bo, s, blk)
            if not kind:
                d = norm2((re, im))
                acc[rows(s % SR, blk), :] += d
                tot[s // SR] += fold(d)
            put(s, re, im, blk)
        loop(size // blk, body)

    sl = lax.broadcasted_iota(jnp.int32, (8, LANES), 0)
    ln = lax.broadcasted_iota(jnp.int32, (8, LANES), 1)

    def sgn(bit):
        return (1 - 2 * bit).astype(jnp.float32)

    def signed(terms, bit):
        parts = [-t if (v >> bit) & 1 else t for v, t in enumerate(terms)]
        while len(parts) > 1:
            parts = [parts[v] + parts[v + 1] for v in range(0, len(parts), 2)]
        return parts[0]

    def sums(half):
        units = [tot[half * NS + v] for v in range(NS)]
        total = signed([t for t in units], 30)
        wide = [acc[8 * v:8 * v + 8, :] for v in range(SR // 8)]
        vecs = [diff[0] * sgn(b), diff[1] * -sgn(b)] if half else [total * sgn(b), total * sgn(z % 2)]
        vecs += [total * sgn(my_bit(4 - q)) for q in range(2, 5)]
        vecs.append(-total if half else total)
        vecs += [signed(units, 10 - q) for q in range(6, 11)]
        vecs += [signed(wide, 14 - q) for q in range(11, 15)]
        vecs += [total * sgn((sl >> (17 - q)) & 1) for q in range(15, 18)]
        vecs += [total * sgn((ln >> (24 - q)) & 1) for q in range(18, 25)]
        parts = [jnp.sum(v, axis=0, keepdims=True) for v in vecs]
        return jnp.concatenate(parts + [jnp.zeros((1, LANES), jnp.float32)] * (32 - NQ), axis=0)

    acc[...] = jnp.zeros_like(acc)
    tot[...] = jnp.zeros_like(tot)
    loop(8, lambda k: emit(0, k))
    fvec[...] = sums(0)
    up_sums = remote(fvec, gvec, vs, vr, dev_in)

    @pl.when(outer)
    def _():
        up_sums.start()

    @pl.when(inner)
    def _():
        def partial(i):
            s = direct(b) + i * BLK
            vals = load(psi, s, BLK), load(abuf, s, BLK)
            store(pm, i * BLK, BLK, cmac(tuple(zip(w_mid, vals))))
            store(pf, i * BLK, BLK, cmac(tuple(zip(w_far, vals))))
        loop(DR // BLK, partial)
        up_sums.wait_recv()
        fvec[...] += gvec[...]
        acc[...] = jnp.zeros_like(acc)
        diff[...] = jnp.zeros_like(diff)

    def phase5(k):
        finish_z(1, k)
        emit(1, k)
    loop(6, phase5)
    for k in (0, 1, 2):
        finish_z(2, k, 4 if k == 2 else 2)
        emit(2, k)
    finish_z(2, 3, 4)

    mine = b * 8 + sub

    def msg_copy(r):
        return remote(msg.at[mine], msg.at[mine], ms, mr, (me + r) % 32)

    @pl.when(inner)
    def _():
        wide = jnp.concatenate([fvec[...] + sums(1), jnp.zeros((LANES - 32, LANES), jnp.float32)], axis=0)
        msg[pl.ds(mine, 1)] = jnp.sum(wide.T, axis=0, keepdims=True)[None]
        loop(31, lambda r: msg_copy(r + 1).start())
        for k in (5, 6):
            send_both(2, k, b)
        for k in range(DR // DP):
            far_copy(k).start()
        for k in range(DR // DP):
            mid_copy(k).start()
    emit(2, 3)
    for k in (4, 5, 6):
        finish_z(2, k, 0)
        emit(2, k)

    @pl.when(outer)
    def _():
        early_copy.wait_recv()
    w_near = [tuple(jnp.where(inner, p, q) for p, q in zip(*pair)) for pair in zip(w_own, (w_out[1], w_out[0]))]
    for k in range(DR // DP):
        mid_copy(k).wait_recv()

        def add_up(i):
            t = k * DP + i * BLK
            s = direct(1 - b) + t
            re, im = cmac(tuple(zip(w_near, (load(psi, s, BLK), load(abuf, s, BLK)))))
            far = load(rp, t, BLK)
            put(s, re + far[0], im + far[1], BLK)
        loop(DP // BLK, add_up)

    def receive(count):
        got = msg.at[pl.ds(0, count)]
        remote(got, got, ms, mr, dev_mid).wait_recv()

    @pl.when(inner)
    def _():
        receive(15)

    @pl.when(outer)
    def _():
        receive(16)
    val = msg[0]
    for t in range(1, 16):
        val = val + msg[t]
    z_ref[...] = (val * (1.0 / (ROWS * LANES * 32)))[:, :NQ]

    @pl.when(inner)
    def _():
        remote(abuf, bf, fs, vr, dev_mid).wait_send()
        remote(sent, sent, ms, vr, dev_mid).wait_send()
        remote(bf, bo, os_, vr, dev_out).wait_send()

    @pl.when(outer)
    def _():
        up_sums.wait_send()
    remote(psi, bo, ps, vr, dev_mid).wait_send()


def writer(s_ref, z_ref, o_hbm, zo_ref, sem):
    copies = [pltpu.make_async_copy(s_ref.at[pl.ds(k * 2 * ROWS // NW, 2 * ROWS // NW), :],
                                    o_hbm.at[pl.ds(k * 2 * ROWS // NW, 2 * ROWS // NW), :], sem.at[k]) for k in range(NW)]
    copies.append(pltpu.make_async_copy(z_ref, zo_ref, sem.at[NW]))
    for cp in copies:
        cp.start()
    for cp in copies:
        cp.wait()


def solution(mesh):
    dma = pltpu.SemaphoreType.DMA
    big = pltpu.VMEM((2, ROWS, LANES), jnp.float32)
    slots = pltpu.VMEM((2, NX * GR, LANES), jnp.float32)

    def local_layer(state_local, unitaries, cz_pairs):
        x = state_local.reshape(2, ROWS, LANES).transpose(1, 0, 2).reshape(2 * ROWS, LANES)
        gates = unitaries.transpose(0, 2, 3, 1)
        out, z_exp = pl.pallas_call(
            kernel,
            name="gate_layer",
            out_shape=(pltpu.VMEM((2 * ROWS, LANES), jnp.float32), pltpu.VMEM((1, NQ), jnp.float32)),
            in_specs=[pl.BlockSpec(memory_space=pl.ANY),
                      pl.BlockSpec(memory_space=pl.ANY),
                      pl.BlockSpec(memory_space=pl.ANY)],
            out_specs=(pl.BlockSpec(memory_space=pltpu.VMEM), pl.BlockSpec(memory_space=pltpu.VMEM)),
            scratch_shapes=[big] * 4 + [slots] * 3 + [
                pltpu.VMEM((4 * 2 * GR, LANES), jnp.float32),
                pltpu.VMEM((256, 256), jnp.float32),
                pltpu.VMEM((256, 256), jnp.float32),
                pltpu.VMEM((SR, LANES), jnp.float32),
                pltpu.VMEM((2 * NS, 8, LANES), jnp.float32),
                pltpu.VMEM((2, 8, LANES), jnp.float32),
                pltpu.VMEM((32, LANES), jnp.float32),
                pltpu.VMEM((32, LANES), jnp.float32),
                pltpu.VMEM((16, 1, LANES), jnp.float32),
                pltpu.VMEM((31, 1, LANES), jnp.float32),
                pltpu.VMEM((2, DR, LANES), jnp.float32),
                pltpu.VMEM((2, DR, LANES), jnp.float32),
                pltpu.VMEM((2, DR, LANES), jnp.float32),
                pltpu.SMEM((2, 2, 2, NQ), jnp.float32),
                pltpu.SMEM((2, 12), jnp.int32),
                dma((2,)), dma((4,)), dma(()), dma((NG,)), dma((NZ,)), dma(()), dma(())] + [
                dma((2,)), dma((NX,))] * 3 + [dma(())] * 5 + [dma((DR // DP,))],
            compiler_params=pltpu.CompilerParams(has_side_effects=True, collective_id=0,
                                                 vmem_limit_bytes=VMEM_LIMIT),
        )(x, gates, cz_pairs.transpose(1, 0))
        out, z_exp = pl.pallas_call(
            writer,
            name="write_result",
            out_shape=(jax.ShapeDtypeStruct((2 * ROWS, LANES), jnp.float32), jax.ShapeDtypeStruct((1, NQ), jnp.float32)),
            in_specs=[pl.BlockSpec(memory_space=pltpu.VMEM), pl.BlockSpec(memory_space=pltpu.VMEM)],
            out_specs=(pl.BlockSpec(memory_space=pl.ANY), pl.BlockSpec(memory_space=pl.ANY)),
            scratch_shapes=[dma((NW + 1,))],
            compiler_params=pltpu.CompilerParams(vmem_limit_bytes=2 ** 20),
        )(out, z_exp)
        out = out.reshape(ROWS, 2, LANES).transpose(1, 0, 2).reshape(2, ROWS * LANES)
        return out, z_exp.reshape(NQ)

    return jax.shard_map(local_layer, mesh=mesh, in_specs=(P(None, 'q'), P(), P()),
                         out_specs=(P(None, 'q'), P()), check_vma=False)
```

```python
import jax
import jax.numpy as jnp
from jax import lax
from jax.experimental import pallas as pl
from jax.experimental.pallas import tpu as pltpu
from jax.sharding import PartitionSpec as P

MESH = pl.DeviceIdType.MESH
LANES = 128
ROWS = 8192
NG = 16
GR = ROWS // NG
PIECES = (256, 128, 64, 64)
DR = GR
DP = 64
ND = DR // DP
NT = len(PIECES)
NZ = NG - 2 + NT
FIRST = 128
SR = 128
NS = 32
HALF = ROWS // 2
BLK = 32
NQ = 25
NW = 8
NX = 4
LO = slice(0, 128)
HI = slice(128, 256)
HIGHEST = lax.Precision.HIGHEST
VMEM_LIMIT = 50 * 2 ** 20


def loop(count, body, unroll=1):
    def step(i, carry):
        body(i)
        return carry
    lax.fori_loop(0, count, step, 0, unroll=unroll)


def cmac(terms):
    out_re = None
    out_im = None
    for (cr, ci), (xr, xi) in terms:
        re = cr * xr - ci * xi
        im = cr * xi + ci * xr
        out_re = re if out_re is None else out_re + re
        out_im = im if out_im is None else out_im + im
    return out_re, out_im


def cprod(a, b):
    return cmac(((a, b),))


def norm2(a):
    re, im = a
    return re * re + im * im


def kernel(x_hbm, u_hbm, cz_hbm, o_ref, z_ref,
           psi, abuf, bo, bf, xb, yb, cb, st, kl, ml, acc, tot, diff, fvec, gvec, msg, sent, pm, pf, rp, u_ref, cz_ref,
           par_sem, in_sem, ps, ar, br, fs, os_, xs, xr, ys, yr, cs, cr_, vs, vr, ms, mr, er, dr):
    me = lax.axis_index('q')
    z = me // 8
    sub = me % 8
    b = z // 2
    inner = jnp.logical_or(z == 1, z == 2)
    outer = jnp.logical_not(inner)
    dev_in = sub + 8 * (1 + b)
    dev_mid = jnp.where(inner, sub + 8 * (3 - z), dev_in)
    dev_out = jnp.where(inner, sub + 24 * b, dev_in)

    def my_bit(k):
        return (me // 2 ** k) % 2

    dev_c, dev_x, dev_y = [me + 2 ** k * (1 - 2 * my_bit(k)) for k in range(3)]

    def in_copy(c, slot, sem, start=0, size=GR):
        return pltpu.make_async_copy(x_hbm.at[pl.ds(pl.multiple_of((c * GR + start) * 2, 8), 2 * size), :],
                                     st.at[pl.ds(pl.multiple_of((slot * GR + start) * 2, 8), 2 * size), :], in_sem.at[sem])

    def in_pair(c, slot, sem, start=0, size=GR):
        return in_copy(c, slot, sem, start, size), in_copy(c + 8, slot + 1, sem + 1, start, size)

    part_a = in_pair(0, 0, 0, 0, FIRST)
    part_b = in_pair(0, 0, 2, FIRST, GR - FIRST)

    barrier = pltpu.get_barrier_semaphore()

    def greet(dev):
        pl.semaphore_signal(barrier, inc=1, device_id=(dev,), device_id_type=MESH)

    greet(dev_x)
    greet(dev_y)
    greet(dev_c)
    greet(dev_mid)

    @pl.when(inner)
    def _():
        greet(dev_out)
    u_copy = pltpu.make_async_copy(u_hbm, u_ref, par_sem.at[0])
    cz_copy = pltpu.make_async_copy(cz_hbm, cz_ref, par_sem.at[1])
    u_copy.start()
    for cp in part_a + part_b:
        cp.start()
    cz_copy.start()
    u_copy.wait()

    def u(q, i, j):
        return u_ref[0, i, j, q], u_ref[1, i, j, q]

    def gate(q):
        return tuple(tuple(u(q, i, j) for j in range(2)) for i in range(2))

    def apply_pair(g, p0, p1):
        return tuple(cmac(tuple(zip(g_row, (p0, p1)))) for g_row in g)

    def rows(start, size):
        return pl.ds(pl.multiple_of(start, 8), size)

    def load(ref, start, size):
        return ref[0, rows(start, size), :], ref[1, rows(start, size), :]

    def store(ref, start, size, val):
        ref[0, rows(start, size), :] = val[0]
        ref[1, rows(start, size), :] = val[1]

    def gslice(ref, c):
        return ref.at[:, rows(c * GR, GR), :]

    def remote(src, dst, ss, rs, dev):
        return pltpu.make_async_remote_copy(src_ref=src, dst_ref=dst, send_sem=ss, recv_sem=rs,
                                            device_id=(dev,), device_id_type=MESH)

    def span(kind, k, hb=0):
        if kind < 2:
            return (kind * 8 + k) * GR, GR
        return (NG - 2 + hb) * GR + sum(PIECES[:k]), PIECES[k]

    def index(kind, k):
        return k + (0, 8, NG - 2)[kind]

    def zcopy(src, dst, ss, rs, dev, place):
        return remote(src.at[:, rows(*place), :], dst.at[:, rows(*place), :], ss, rs, dev)

    def own_copy(kind, k, place):
        return zcopy(psi, bo, ps, br.at[index(kind, k)], dev_mid, place)

    def up_copy(c, place):
        return zcopy(psi, abuf, ps, ar.at[c], dev_in, place)

    def fwd_copy(kind, k, place):
        return zcopy(abuf, bf, fs, br.at[index(kind, k)], dev_mid, place)

    def down_copy(kind, k, place):
        return zcopy(bf, bo, os_, br.at[index(kind, k)], dev_out, place)

    def direct(hb):
        return (NG - 1 - hb) * GR

    early_copy = zcopy(psi, abuf, ps, er, dev_out, (direct(1 - b), DR))
    dev_far = sub + 24 * (1 - b)

    def part(ref, k):
        return ref.at[:, rows(k * DP, DP), :]

    def far_copy(k):
        return remote(part(pf, k), part(rp, k), os_, dr.at[k], dev_far)

    def mid_copy(k):
        return remote(part(pm, k), part(rp, k), fs, dr.at[k], dev_mid)

    def send_both(kind, k, hb=0):
        own_copy(kind, k, span(kind, k, hb)).start()
        fwd_copy(kind, k, span(kind, k, hb)).start()

    g5 = gate(5)

    def gate5(c, slot, start=0, size=GR):
        def body(i):
            r = start + i * BLK
            s0 = (slot * GR + r) * 2
            s1 = s0 + 2 * GR
            lo = st[pl.ds(s0, BLK, stride=2), :], st[pl.ds(s0 + 1, BLK, stride=2), :]
            hi = st[pl.ds(s1, BLK, stride=2), :], st[pl.ds(s1 + 1, BLK, stride=2), :]
            n0, n1 = apply_pair(g5, lo, hi)
            store(psi, c * GR + r, BLK, n0)
            store(psi, (c + 8) * GR + r, BLK, n1)
        loop(size // BLK, body)

    def send_first(c, start=0, size=GR):
        place = (c * GR + start, size)

        @pl.when(inner)
        def _():
            own_copy(0, c, place).start()

        @pl.when(outer)
        def _():
            up_copy(c, place).start()

    for cp in part_a:
        cp.wait()
    gate5(0, 0, 0, FIRST)

    @pl.when(inner)
    def _():
        pl.semaphore_wait(barrier, 5)

    @pl.when(outer)
    def _():
        pl.semaphore_wait(barrier, 4)
    send_first(0, 0, FIRST)
    for cp in part_b:
        cp.wait()
    for cp in in_pair(1, 2, 2):
        cp.start()
    gate5(0, 0, FIRST, GR - FIRST)
    send_first(0, FIRST, GR - FIRST)

    def phase0(m):
        c = m + 1
        slot = 2 * (c % 2)
        nxt = 2 - slot

        @pl.when(c < 7)
        def _():
            for cp in in_pair(c + 1, nxt, nxt):
                cp.start()
        for cp in in_pair(c, slot, slot):
            cp.wait()
        gate5(c, slot)
        send_first(c)
    loop(7, phase0)
    cz_copy.wait()
    def z_row(hi, lo):
        return [cprod(u(0, hi, v), u(1, lo, w)) for v, w in ((b, 1 - b), (b, b), (1 - b, b), (1 - b, 1 - b))]
    w_own = z_row(b, 1 - b)
    w_out = z_row(b, b)
    w_mid = z_row(1 - b, b)
    w_far = z_row(1 - b, 1 - b)

    def fold(d):
        t = d[0:8]
        for j in range(1, d.shape[0] // 8):
            t = t + d[8 * j:8 * j + 8]
        return t

    def finish_z(kind, k, count=2):
        start, size = span(kind, k, 1 - b)
        blk = min(BLK, size)

        @pl.when(inner)
        def _():
            zcopy(psi, bo, ps, br.at[index(kind, k)], dev_mid, (0, 2 * size)).wait_recv()

            def body(i):
                s = start + i * blk
                vals = (load(psi, s, blk), load(abuf, s, blk), load(bo, s, blk), load(bf, s, blk))
                own = cmac(tuple(zip(w_own, vals)))
                out = cmac(tuple(zip(w_out, vals)))
                store(bf, s, blk, out)
                store(bo, s, blk, own)
                if kind and count:
                    d_own = norm2(own)
                    d_out = norm2(out)
                    near = d_own + d_out
                    d0, d1 = near, d_own - d_out
                    if count == 4:
                        d_mid = norm2(cmac(tuple(zip(w_mid, vals))))
                        d_far = norm2(cmac(tuple(zip(w_far, vals))))
                        d0, d1 = near - (d_mid + d_far), d1 + (d_far - d_mid)
                        near = near + (d_mid + d_far)
                    acc[rows(s % SR, blk), :] += near
                    tot[s // SR] += fold(near)
                    diff[0] += fold(d0)
                    diff[1] += fold(d1)
            loop(size // blk, body)
            down_copy(kind, k, (start, size)).start()

        @pl.when(outer)
        def _():
            down_copy(kind, k, (start, size)).wait_recv()

    def xchg(state, c, stage):
        buf, ss, rs, dev = ((xb, xs, xr, dev_x), (yb, ys, yr, dev_y), (cb, cs, cr_, dev_c))[stage]
        return remote(gslice(state, c), gslice(buf, c % NX), ss.at[c % 2], rs.at[c % NX], dev)

    bits = [my_bit(k) for k in (1, 2, 0)]
    mix_coef = tuple((u(q, v, v), u(q, v, 1 - v)) for q, v in zip((3, 2, 4), bits))

    def mix(state, c, stage):
        cp = xchg(state, c, stage)
        cp.wait_send()
        cp.wait_recv()
        other = (xb, yb, cb)[stage]
        coef = mix_coef[stage]

        def body(i):
            s = c * GR + i * BLK
            t = (c % NX) * GR + i * BLK
            store(state, s, BLK, cmac(((coef[0], load(state, s, BLK)), (coef[1], load(other, t, BLK)))))
        loop(GR // BLK, body, unroll=2)

    g9 = gate(9)
    g10 = gate(10)

    def local_gates(state, c):
        base = c * GR

        def rowgates(i):
            p = [load(state, base + j * 128 + i * 16, 16) for j in range(4)]
            for g, step in ((g9, 2), (g10, 1)):
                for j in range(4):
                    if not j & step:
                        p[j], p[j + step] = apply_pair(g, p[j], p[j + step])
            for j in range(4):
                store(state, base + j * 128 + i * 16, 16, p[j])
        loop(8, rowgates)

        def mats(h):
            s = base + h * 256
            a = load(state, s, 128)
            d = load(state, s + 128, 128)
            packed = jnp.concatenate([jnp.concatenate(pair, axis=1) for pair in zip(a, d)], axis=0)
            m = jnp.dot(ml[...], packed, precision=HIGHEST, preferred_element_type=jnp.float32)
            packed = jnp.concatenate([jnp.concatenate([m[LO, h], m[HI, h]], axis=1) for h in (LO, HI)], axis=0)
            m = jnp.dot(packed, kl[...], precision=HIGHEST, preferred_element_type=jnp.float32)
            store(state, s, 256, (m[:, LO], m[:, HI]))
        loop(2, mats)

    g678 = (gate(6), gate(7), gate(8))

    def chunk_gates(state, first_row):
        def body(i):
            p = [load(state, first_row + j * GR + i * 8, 8) for j in range(8)]
            for g, step in zip(g678, (4, 2, 1)):
                for j in range(8):
                    if not j & step:
                        p[j], p[j + step] = apply_pair(g, p[j], p[j + step])
            for j in range(8):
                store(state, first_row + j * GR + i * 8, 8, p[j])
        loop(GR // 8, body)

    row = lax.broadcasted_iota(jnp.int32, (128, 128), 0)
    col = lax.broadcasted_iota(jnp.int32, (128, 128), 1)

    def kron(first, out_idx, in_idx):
        val = None
        for j in range(7):
            g = gate(first + j)
            ob = ((out_idx >> (6 - j)) & 1) == 1
            ib = ((in_idx >> (6 - j)) & 1) == 1
            f = tuple(jnp.where(ob, jnp.where(ib, g[1][1][r], g[1][0][r]), jnp.where(ib, g[0][1][r], g[0][0][r]))
                      for r in range(2))
            val = f if val is None else cprod(val, f)
        return val
    km = kron(18, col, row)
    kl[LO, LO] = km[0]
    kl[LO, HI] = km[1]
    kl[HI, LO] = -km[1]
    kl[HI, HI] = km[0]
    mm = kron(11, row, col)
    ml[LO, LO] = mm[0]
    ml[LO, HI] = -mm[1]
    ml[HI, LO] = mm[1]
    ml[HI, HI] = mm[0]
    chunk_gates(psi, HALF)

    def phase2(i):
        @pl.when(i < 8)
        def _():
            local_gates(psi, 8 + i)
            xchg(psi, 8 + i, 0).start()

            @pl.when(inner)
            def _():
                up_copy(i, span(0, i)).wait_recv()
                fwd_copy(0, i, span(0, i)).start()

        @pl.when(jnp.logical_and(i >= 1, i < 9))
        def _():
            mix(psi, 7 + i, 0)
            xchg(psi, 7 + i, 1).start()

        @pl.when(jnp.logical_and(i >= 2, i < 10))
        def _():
            mix(psi, 6 + i, 1)
            xchg(psi, 6 + i, 2).start()

        @pl.when(i >= 3)
        def _():
            mix(psi, 5 + i, 2)

            @pl.when(outer)
            def _():
                up_copy(5 + i, span(1, i - 3)).start()
    loop(11, phase2)

    def phase3(i):
        @pl.when(i < 8)
        def _():
            @pl.when(inner)
            def _():
                @pl.when(i < 6)
                def _():
                    own_copy(1, i, span(1, i)).start()
                    up_copy(8 + i, span(1, i)).wait_recv()
                    fwd_copy(1, i, span(1, i)).start()

                @pl.when(i == 7)
                def _():
                    for k in (6, 7):
                        up_copy(8 + k, span(1, k)).wait_recv()

                    def partial(j):
                        s = direct(b) + j * BLK
                        vals = load(psi, s, BLK), load(abuf, s, BLK)
                        store(pm, j * BLK, BLK, cmac(tuple(zip(w_mid, vals))))
                        store(pf, j * BLK, BLK, cmac(tuple(zip(w_far, vals))))
                    loop(DR // BLK, partial)
                    loop(ND, lambda k: far_copy(k).start())
                    for k in range(NT):
                        send_both(2, k, b)
                    mid_copy(0).start()
                    early_copy.start()
            finish_z(0, i)
            local_gates(bo, i)
            xchg(bo, i, 0).start()

        @pl.when(jnp.logical_and(i >= 1, i < 9))
        def _():
            mix(bo, i - 1, 0)
            xchg(bo, i - 1, 1).start()

        @pl.when(jnp.logical_and(i >= 2, i < 10))
        def _():
            mix(bo, i - 2, 1)
            xchg(bo, i - 2, 2).start()

        @pl.when(i >= 3)
        def _():
            mix(bo, i - 3, 2)
    loop(11, phase3)

    chunk_gates(bo, 0)
    flat = lax.broadcasted_iota(jnp.int32, (BLK, LANES), 0) * LANES + lax.broadcasted_iota(jnp.int32, (BLK, LANES), 1)
    shifts = [(NQ - 1 - cz_ref[0, p], NQ - 1 - cz_ref[1, p]) for p in range(12)]

    def put(s, re, im, blk):
        idx = flat[:blk] + (me * (ROWS * LANES) + s * LANES)
        par = None
        for sa, sb in shifts:
            t = lax.shift_right_logical(idx, sa) & lax.shift_right_logical(idx, sb)
            par = t if par is None else par ^ t
        sign = (1 - 2 * (par & 1)).astype(jnp.float32)
        o_ref[pl.ds(2 * s, blk, stride=2), :] = re * sign
        o_ref[pl.ds(2 * s + 1, blk, stride=2), :] = im * sign

    def emit(kind, k):
        start, size = span(kind, k, 1 - b)
        blk = min(BLK, size)

        def body(i):
            s = start + i * blk
            re, im = load(bo, s, blk)
            if not kind:
                d = norm2((re, im))
                acc[rows(s % SR, blk), :] += d
                tot[s // SR] += fold(d)
            put(s, re, im, blk)
        loop(size // blk, body)

    sl = lax.broadcasted_iota(jnp.int32, (8, LANES), 0)
    ln = lax.broadcasted_iota(jnp.int32, (8, LANES), 1)

    def sgn(bit):
        return (1 - 2 * bit).astype(jnp.float32)

    def signed(terms, bit):
        parts = [-t if (v >> bit) & 1 else t for v, t in enumerate(terms)]
        while len(parts) > 1:
            parts = [parts[v] + parts[v + 1] for v in range(0, len(parts), 2)]
        return parts[0]

    def sums(half):
        units = [tot[half * NS + v] for v in range(NS)]
        total = signed([t for t in units], 30)
        wide = [acc[8 * v:8 * v + 8, :] for v in range(SR // 8)]
        vecs = [diff[0] * sgn(b), diff[1] * -sgn(b)] if half else [total * sgn(b), total * sgn(z % 2)]
        vecs += [total * sgn(my_bit(4 - q)) for q in range(2, 5)]
        vecs.append(-total if half else total)
        vecs += [signed(units, 10 - q) for q in range(6, 11)]
        vecs += [signed(wide, 14 - q) for q in range(11, 15)]
        vecs += [total * sgn((sl >> (17 - q)) & 1) for q in range(15, 18)]
        vecs += [total * sgn((ln >> (24 - q)) & 1) for q in range(18, 25)]
        parts = [jnp.sum(v, axis=0, keepdims=True) for v in vecs]
        return jnp.concatenate(parts + [jnp.zeros((1, LANES), jnp.float32)] * (32 - NQ), axis=0)

    acc[...] = jnp.zeros_like(acc)
    tot[...] = jnp.zeros_like(tot)
    loop(8, lambda k: emit(0, k))
    fvec[...] = sums(0)
    up_sums = remote(fvec, gvec, vs, vr, dev_in)

    @pl.when(outer)
    def _():
        up_sums.start()

    @pl.when(inner)
    def _():
        up_sums.wait_recv()
        fvec[...] += gvec[...]
        acc[...] = jnp.zeros_like(acc)
        diff[...] = jnp.zeros_like(diff)

    def phase5(k):
        finish_z(1, k)
        emit(1, k)
    loop(6, phase5)
    for k in range(NT - 1):
        finish_z(2, k, 4)
        emit(2, k)
    finish_z(2, NT - 1, 4)

    mine = b * 8 + sub

    def msg_copy(r):
        return remote(msg.at[mine], msg.at[mine], ms, mr, (me + r) % 32)

    @pl.when(inner)
    def _():
        wide = jnp.concatenate([fvec[...] + sums(1), jnp.zeros((LANES - 32, LANES), jnp.float32)], axis=0)
        msg[pl.ds(mine, 1)] = jnp.sum(wide.T, axis=0, keepdims=True)[None]
        loop(31, lambda r: msg_copy(r + 1).start())
        loop(ND - 1, lambda k: mid_copy(k + 1).start())
    emit(2, NT - 1)

    @pl.when(outer)
    def _():
        early_copy.wait_recv()
    w_near = [tuple(jnp.where(inner, p, q) for p, q in zip(*pair)) for pair in zip(w_own, (w_out[1], w_out[0]))]

    def take(k):
        mid_copy(k).wait_recv()

        def add_up(i):
            t = k * DP + i * BLK
            s = direct(1 - b) + t
            re, im = cmac(tuple(zip(w_near, (load(psi, s, BLK), load(abuf, s, BLK)))))
            far = load(rp, t, BLK)
            put(s, re + far[0], im + far[1], BLK)
        loop(DP // BLK, add_up)
    loop(ND, take)

    def receive(count):
        got = msg.at[pl.ds(0, count)]
        remote(got, got, ms, mr, dev_mid).wait_recv()

    @pl.when(inner)
    def _():
        receive(15)

    @pl.when(outer)
    def _():
        receive(16)
    val = msg[0]
    for t in range(1, 16):
        val = val + msg[t]
    z_ref[...] = (val * (1.0 / (ROWS * LANES * 32)))[:, :NQ]

    @pl.when(inner)
    def _():
        remote(abuf, bf, fs, vr, dev_mid).wait_send()
        remote(sent, sent, ms, vr, dev_mid).wait_send()
        remote(bf, bo, os_, vr, dev_out).wait_send()

    @pl.when(outer)
    def _():
        up_sums.wait_send()
    remote(psi, bo, ps, vr, dev_mid).wait_send()


def writer(s_ref, z_ref, o_hbm, zo_ref, sem):
    copies = [pltpu.make_async_copy(s_ref.at[pl.ds(k * 2 * ROWS // NW, 2 * ROWS // NW), :],
                                    o_hbm.at[pl.ds(k * 2 * ROWS // NW, 2 * ROWS // NW), :], sem.at[k]) for k in range(NW)]
    copies.append(pltpu.make_async_copy(z_ref, zo_ref, sem.at[NW]))
    for cp in copies:
        cp.start()
    for cp in copies:
        cp.wait()


def solution(mesh):
    dma = pltpu.SemaphoreType.DMA
    big = pltpu.VMEM((2, ROWS, LANES), jnp.float32)
    slots = pltpu.VMEM((2, NX * GR, LANES), jnp.float32)

    def local_layer(state_local, unitaries, cz_pairs):
        x = state_local.reshape(2, ROWS, LANES).transpose(1, 0, 2).reshape(2 * ROWS, LANES)
        gates = unitaries.transpose(0, 2, 3, 1)
        out, z_exp = pl.pallas_call(
            kernel,
            name="gate_layer",
            out_shape=(pltpu.VMEM((2 * ROWS, LANES), jnp.float32), pltpu.VMEM((1, NQ), jnp.float32)),
            in_specs=[pl.BlockSpec(memory_space=pl.ANY),
                      pl.BlockSpec(memory_space=pl.ANY),
                      pl.BlockSpec(memory_space=pl.ANY)],
            out_specs=(pl.BlockSpec(memory_space=pltpu.VMEM), pl.BlockSpec(memory_space=pltpu.VMEM)),
            scratch_shapes=[big] * 4 + [slots] * 3 + [
                pltpu.VMEM((4 * 2 * GR, LANES), jnp.float32),
                pltpu.VMEM((256, 256), jnp.float32),
                pltpu.VMEM((256, 256), jnp.float32),
                pltpu.VMEM((SR, LANES), jnp.float32),
                pltpu.VMEM((2 * NS, 8, LANES), jnp.float32),
                pltpu.VMEM((2, 8, LANES), jnp.float32),
                pltpu.VMEM((32, LANES), jnp.float32),
                pltpu.VMEM((32, LANES), jnp.float32),
                pltpu.VMEM((16, 1, LANES), jnp.float32),
                pltpu.VMEM((31, 1, LANES), jnp.float32),
                pltpu.VMEM((2, DR, LANES), jnp.float32),
                pltpu.VMEM((2, DR, LANES), jnp.float32),
                pltpu.VMEM((2, DR, LANES), jnp.float32),
                pltpu.SMEM((2, 2, 2, NQ), jnp.float32),
                pltpu.SMEM((2, 12), jnp.int32),
                dma((2,)), dma((4,)), dma(()), dma((NG,)), dma((NZ,)), dma(()), dma(())] + [
                dma((2,)), dma((NX,))] * 3 + [dma(())] * 5 + [dma((ND,))],
            compiler_params=pltpu.CompilerParams(has_side_effects=True, collective_id=0,
                                                 vmem_limit_bytes=VMEM_LIMIT),
        )(x, gates, cz_pairs.transpose(1, 0))
        out, z_exp = pl.pallas_call(
            writer,
            name="write_result",
            out_shape=(jax.ShapeDtypeStruct((2 * ROWS, LANES), jnp.float32), jax.ShapeDtypeStruct((1, NQ), jnp.float32)),
            in_specs=[pl.BlockSpec(memory_space=pltpu.VMEM), pl.BlockSpec(memory_space=pltpu.VMEM)],
            out_specs=(pl.BlockSpec(memory_space=pl.ANY), pl.BlockSpec(memory_space=pl.ANY)),
            scratch_shapes=[dma((NW + 1,))],
            compiler_params=pltpu.CompilerParams(vmem_limit_bytes=2 ** 20),
        )(out, z_exp)
        out = out.reshape(ROWS, 2, LANES).transpose(1, 0, 2).reshape(2, ROWS * LANES)
        return out, z_exp.reshape(NQ)

    return jax.shard_map(local_layer, mesh=mesh, in_specs=(P(None, 'q'), P(), P()),
                         out_specs=(P(None, 'q'), P()), check_vma=False)
```

```python
import jax
import jax.numpy as jnp
from jax import lax
from jax.experimental import pallas as pl
from jax.experimental.pallas import tpu as pltpu
from jax.sharding import PartitionSpec as P

MESH = pl.DeviceIdType.MESH
LANES = 128
ROWS = 8192
NG = 16
GR = ROWS // NG
PIECES = (256, 128, 64, 64)
DR = GR
DP = 64
ND = DR // DP
NT = len(PIECES)
NZ = NG - 2 + NT
FIRST = 64
SR = 128
NS = 32
HALF = ROWS // 2
BLK = 32
NQ = 25
NW = 8
NX = 4
LO = slice(0, 128)
HI = slice(128, 256)
HIGHEST = lax.Precision.HIGHEST
VMEM_LIMIT = 50 * 2 ** 20


def loop(count, body, unroll=1):
    def step(i, carry):
        body(i)
        return carry
    lax.fori_loop(0, count, step, 0, unroll=unroll)


def cmac(terms):
    out_re = None
    out_im = None
    for (cr, ci), (xr, xi) in terms:
        re = cr * xr - ci * xi
        im = cr * xi + ci * xr
        out_re = re if out_re is None else out_re + re
        out_im = im if out_im is None else out_im + im
    return out_re, out_im


def cprod(a, b):
    return cmac(((a, b),))


def norm2(a):
    re, im = a
    return re * re + im * im


def kernel(x_hbm, u_hbm, cz_hbm, o_ref, z_ref,
           psi, abuf, bo, bf, xb, yb, cb, st, kl, ml, acc, tot, diff, fvec, gvec, msg, sent, pm, pf, rp, u_ref, cz_ref,
           par_sem, in_sem, ps, ar, br, fs, os_, xs, xr, ys, yr, cs, cr_, vs, vr, ms, mr, er, dr):
    me = lax.axis_index('q')
    z = me // 8
    sub = me % 8
    b = z // 2
    inner = jnp.logical_or(z == 1, z == 2)
    outer = jnp.logical_not(inner)
    dev_in = sub + 8 * (1 + b)
    dev_mid = jnp.where(inner, sub + 8 * (3 - z), dev_in)
    dev_out = jnp.where(inner, sub + 24 * b, dev_in)

    def my_bit(k):
        return (me // 2 ** k) % 2

    dev_c, dev_x, dev_y = [me + 2 ** k * (1 - 2 * my_bit(k)) for k in range(3)]

    def in_copy(c, slot, sem, start=0, size=GR):
        return pltpu.make_async_copy(x_hbm.at[pl.ds(pl.multiple_of((c * GR + start) * 2, 8), 2 * size), :],
                                     st.at[pl.ds(pl.multiple_of((slot * GR + start) * 2, 8), 2 * size), :], in_sem.at[sem])

    def in_pair(c, slot, sem, start=0, size=GR):
        return in_copy(c, slot, sem, start, size), in_copy(c + 8, slot + 1, sem + 1, start, size)

    part_a = in_pair(0, 0, 0, 0, FIRST)
    part_b = in_pair(0, 0, 2, FIRST, GR - FIRST)

    barrier = pltpu.get_barrier_semaphore()

    def greet(dev):
        pl.semaphore_signal(barrier, inc=1, device_id=(dev,), device_id_type=MESH)

    @pl.when(inner)
    def _():
        greet(dev_mid)
        greet(dev_out)
    greet(dev_y)
    greet(dev_x)
    greet(dev_c)
    u_copy = pltpu.make_async_copy(u_hbm, u_ref, par_sem.at[0])
    cz_copy = pltpu.make_async_copy(cz_hbm, cz_ref, par_sem.at[1])
    u_copy.start()
    for cp in part_a + part_b:
        cp.start()
    cz_copy.start()
    u_copy.wait()

    def u(q, i, j):
        return u_ref[0, i, j, q], u_ref[1, i, j, q]

    def gate(q):
        return tuple(tuple(u(q, i, j) for j in range(2)) for i in range(2))

    def apply_pair(g, p0, p1):
        return tuple(cmac(tuple(zip(g_row, (p0, p1)))) for g_row in g)

    def rows(start, size):
        return pl.ds(pl.multiple_of(start, 8), size)

    def load(ref, start, size):
        return ref[0, rows(start, size), :], ref[1, rows(start, size), :]

    def store(ref, start, size, val):
        ref[0, rows(start, size), :] = val[0]
        ref[1, rows(start, size), :] = val[1]

    def gslice(ref, c):
        return ref.at[:, rows(c * GR, GR), :]

    def remote(src, dst, ss, rs, dev):
        return pltpu.make_async_remote_copy(src_ref=src, dst_ref=dst, send_sem=ss, recv_sem=rs,
                                            device_id=(dev,), device_id_type=MESH)

    def span(kind, k, hb=0):
        if kind < 2:
            return (kind * 8 + k) * GR, GR
        return (NG - 2 + hb) * GR + sum(PIECES[:k]), PIECES[k]

    def index(kind, k):
        return k + (0, 8, NG - 2)[kind]

    def zcopy(src, dst, ss, rs, dev, place):
        return remote(src.at[:, rows(*place), :], dst.at[:, rows(*place), :], ss, rs, dev)

    def own_copy(kind, k, place):
        return zcopy(psi, bo, ps, br.at[index(kind, k)], dev_mid, place)

    def up_copy(c, place):
        return zcopy(psi, abuf, ps, ar.at[c], dev_in, place)

    def fwd_copy(kind, k, place):
        return zcopy(abuf, bf, fs, br.at[index(kind, k)], dev_mid, place)

    def down_copy(kind, k, place):
        return zcopy(bf, bo, os_, br.at[index(kind, k)], dev_out, place)

    def direct(hb):
        return (NG - 1 - hb) * GR

    early_copy = zcopy(psi, abuf, ps, er, dev_out, (direct(1 - b), DR))
    dev_far = sub + 24 * (1 - b)

    def part(ref, k):
        return ref.at[:, rows(k * DP, DP), :]

    def far_copy(k):
        return remote(part(pf, k), part(rp, k), os_, dr.at[k], dev_far)

    def mid_copy(k):
        return remote(part(pm, k), part(rp, k), fs, dr.at[k], dev_mid)

    def send_both(kind, k, hb=0):
        own_copy(kind, k, span(kind, k, hb)).start()
        fwd_copy(kind, k, span(kind, k, hb)).start()

    g5 = gate(5)

    def gate5(c, slot, start=0, size=GR):
        def body(i):
            r = start + i * BLK
            s0 = (slot * GR + r) * 2
            s1 = s0 + 2 * GR
            lo = st[pl.ds(s0, BLK, stride=2), :], st[pl.ds(s0 + 1, BLK, stride=2), :]
            hi = st[pl.ds(s1, BLK, stride=2), :], st[pl.ds(s1 + 1, BLK, stride=2), :]
            n0, n1 = apply_pair(g5, lo, hi)
            store(psi, c * GR + r, BLK, n0)
            store(psi, (c + 8) * GR + r, BLK, n1)
        loop(size // BLK, body)

    def send_first(c, start=0, size=GR):
        place = (c * GR + start, size)

        @pl.when(inner)
        def _():
            own_copy(0, c, place).start()

        @pl.when(outer)
        def _():
            up_copy(c, place).start()

    for cp in part_a:
        cp.wait()
    gate5(0, 0, 0, FIRST)

    pl.semaphore_wait(barrier, 4)
    send_first(0, 0, FIRST)
    for cp in part_b:
        cp.wait()
    for cp in in_pair(1, 2, 2):
        cp.start()
    gate5(0, 0, FIRST, GR - FIRST)
    send_first(0, FIRST, GR - FIRST)

    def phase0(m):
        c = m + 1
        slot = 2 * (c % 2)
        nxt = 2 - slot

        @pl.when(c < 7)
        def _():
            for cp in in_pair(c + 1, nxt, nxt):
                cp.start()
        for cp in in_pair(c, slot, slot):
            cp.wait()
        gate5(c, slot)
        send_first(c)
    loop(7, phase0)
    cz_copy.wait()
    def z_row(hi, lo):
        return [cprod(u(0, hi, v), u(1, lo, w)) for v, w in ((b, 1 - b), (b, b), (1 - b, b), (1 - b, 1 - b))]
    w_own = z_row(b, 1 - b)
    w_out = z_row(b, b)
    w_mid = z_row(1 - b, b)
    w_far = z_row(1 - b, 1 - b)

    def fold(d):
        t = d[0:8]
        for j in range(1, d.shape[0] // 8):
            t = t + d[8 * j:8 * j + 8]
        return t

    def finish_z(kind, k, count=2):
        start, size = span(kind, k, 1 - b)
        blk = min(BLK, size)

        @pl.when(inner)
        def _():
            zcopy(psi, bo, ps, br.at[index(kind, k)], dev_mid, (0, 2 * size)).wait_recv()

            def body(i):
                s = start + i * blk
                vals = (load(psi, s, blk), load(abuf, s, blk), load(bo, s, blk), load(bf, s, blk))
                own = cmac(tuple(zip(w_own, vals)))
                out = cmac(tuple(zip(w_out, vals)))
                store(bf, s, blk, out)
                store(bo, s, blk, own)
                if kind and count:
                    d_own = norm2(own)
                    d_out = norm2(out)
                    near = d_own + d_out
                    d0, d1 = near, d_own - d_out
                    if count == 4:
                        d_mid = norm2(cmac(tuple(zip(w_mid, vals))))
                        d_far = norm2(cmac(tuple(zip(w_far, vals))))
                        d0, d1 = near - (d_mid + d_far), d1 + (d_far - d_mid)
                        near = near + (d_mid + d_far)
                    acc[rows(s % SR, blk), :] += near
                    tot[s // SR] += fold(near)
                    diff[0] += fold(d0)
                    diff[1] += fold(d1)
            loop(size // blk, body)
            down_copy(kind, k, (start, size)).start()

        @pl.when(outer)
        def _():
            down_copy(kind, k, (start, size)).wait_recv()

    def xchg(state, c, stage):
        buf, ss, rs, dev = ((xb, xs, xr, dev_x), (yb, ys, yr, dev_y), (cb, cs, cr_, dev_c))[stage]
        return remote(gslice(state, c), gslice(buf, c % NX), ss.at[c % 2], rs.at[c % NX], dev)

    bits = [my_bit(k) for k in (1, 2, 0)]
    mix_coef = tuple((u(q, v, v), u(q, v, 1 - v)) for q, v in zip((3, 2, 4), bits))

    def mix(state, c, stage):
        cp = xchg(state, c, stage)
        cp.wait_send()
        cp.wait_recv()
        other = (xb, yb, cb)[stage]
        coef = mix_coef[stage]

        def body(i):
            s = c * GR + i * BLK
            t = (c % NX) * GR + i * BLK
            store(state, s, BLK, cmac(((coef[0], load(state, s, BLK)), (coef[1], load(other, t, BLK)))))
        loop(GR // BLK, body, unroll=2)

    g9 = gate(9)
    g10 = gate(10)

    def local_gates(state, c):
        base = c * GR

        def rowgates(i):
            p = [load(state, base + j * 128 + i * 16, 16) for j in range(4)]
            for g, step in ((g9, 2), (g10, 1)):
                for j in range(4):
                    if not j & step:
                        p[j], p[j + step] = apply_pair(g, p[j], p[j + step])
            for j in range(4):
                store(state, base + j * 128 + i * 16, 16, p[j])
        loop(8, rowgates)

        def mats(h):
            s = base + h * 256
            a = load(state, s, 128)
            d = load(state, s + 128, 128)
            packed = jnp.concatenate([jnp.concatenate(pair, axis=1) for pair in zip(a, d)], axis=0)
            m = jnp.dot(ml[...], packed, precision=HIGHEST, preferred_element_type=jnp.float32)
            packed = jnp.concatenate([jnp.concatenate([m[LO, h], m[HI, h]], axis=1) for h in (LO, HI)], axis=0)
            m = jnp.dot(packed, kl[...], precision=HIGHEST, preferred_element_type=jnp.float32)
            store(state, s, 256, (m[:, LO], m[:, HI]))
        loop(2, mats)

    g678 = (gate(6), gate(7), gate(8))

    def chunk_gates(state, first_row):
        def body(i):
            p = [load(state, first_row + j * GR + i * 8, 8) for j in range(8)]
            for g, step in zip(g678, (4, 2, 1)):
                for j in range(8):
                    if not j & step:
                        p[j], p[j + step] = apply_pair(g, p[j], p[j + step])
            for j in range(8):
                store(state, first_row + j * GR + i * 8, 8, p[j])
        loop(GR // 8, body)

    row = lax.broadcasted_iota(jnp.int32, (128, 128), 0)
    col = lax.broadcasted_iota(jnp.int32, (128, 128), 1)

    def kron(first, out_idx, in_idx):
        val = None
        for j in range(7):
            g = gate(first + j)
            ob = ((out_idx >> (6 - j)) & 1) == 1
            ib = ((in_idx >> (6 - j)) & 1) == 1
            f = tuple(jnp.where(ob, jnp.where(ib, g[1][1][r], g[1][0][r]), jnp.where(ib, g[0][1][r], g[0][0][r]))
                      for r in range(2))
            val = f if val is None else cprod(val, f)
        return val
    km = kron(18, col, row)
    kl[LO, LO] = km[0]
    kl[LO, HI] = km[1]
    kl[HI, LO] = -km[1]
    kl[HI, HI] = km[0]
    mm = kron(11, row, col)
    ml[LO, LO] = mm[0]
    ml[LO, HI] = -mm[1]
    ml[HI, LO] = mm[1]
    ml[HI, HI] = mm[0]
    chunk_gates(psi, HALF)

    def phase2(i):
        @pl.when(i < 8)
        def _():
            local_gates(psi, 8 + i)
            xchg(psi, 8 + i, 0).start()

            @pl.when(inner)
            def _():
                up_copy(i, span(0, i)).wait_recv()
                fwd_copy(0, i, span(0, i)).start()

        @pl.when(jnp.logical_and(i >= 1, i < 9))
        def _():
            mix(psi, 7 + i, 0)
            xchg(psi, 7 + i, 1).start()

        @pl.when(jnp.logical_and(i >= 2, i < 10))
        def _():
            mix(psi, 6 + i, 1)
            xchg(psi, 6 + i, 2).start()

        @pl.when(i >= 3)
        def _():
            mix(psi, 5 + i, 2)

            @pl.when(outer)
            def _():
                up_copy(5 + i, span(1, i - 3)).start()
    loop(11, phase2)

    def phase3(i):
        @pl.when(i < 8)
        def _():
            @pl.when(inner)
            def _():
                @pl.when(i < 6)
                def _():
                    own_copy(1, i, span(1, i)).start()
                    up_copy(8 + i, span(1, i)).wait_recv()
                    fwd_copy(1, i, span(1, i)).start()

                @pl.when(i == 7)
                def _():
                    for k in (6, 7):
                        up_copy(8 + k, span(1, k)).wait_recv()

                    def partial(j):
                        s = direct(b) + j * BLK
                        vals = load(psi, s, BLK), load(abuf, s, BLK)
                        store(pm, j * BLK, BLK, cmac(tuple(zip(w_mid, vals))))
                        store(pf, j * BLK, BLK, cmac(tuple(zip(w_far, vals))))
                    loop(DR // BLK, partial)
                    loop(ND, lambda k: far_copy(k).start())
                    for k in range(NT):
                        send_both(2, k, b)
                    mid_copy(0).start()
                    early_copy.start()
            finish_z(0, i)
            local_gates(bo, i)
            xchg(bo, i, 0).start()

        @pl.when(jnp.logical_and(i >= 1, i < 9))
        def _():
            mix(bo, i - 1, 0)
            xchg(bo, i - 1, 1).start()

        @pl.when(jnp.logical_and(i >= 2, i < 10))
        def _():
            mix(bo, i - 2, 1)
            xchg(bo, i - 2, 2).start()

        @pl.when(i >= 3)
        def _():
            mix(bo, i - 3, 2)
    loop(11, phase3)

    chunk_gates(bo, 0)
    flat = lax.broadcasted_iota(jnp.int32, (BLK, LANES), 0) * LANES + lax.broadcasted_iota(jnp.int32, (BLK, LANES), 1)
    shifts = [(NQ - 1 - cz_ref[0, p], NQ - 1 - cz_ref[1, p]) for p in range(12)]

    def put(s, re, im, blk):
        idx = flat[:blk] + (me * (ROWS * LANES) + s * LANES)
        par = None
        for sa, sb in shifts:
            t = lax.shift_right_logical(idx, sa) & lax.shift_right_logical(idx, sb)
            par = t if par is None else par ^ t
        sign = (1 - 2 * (par & 1)).astype(jnp.float32)
        o_ref[pl.ds(2 * s, blk, stride=2), :] = re * sign
        o_ref[pl.ds(2 * s + 1, blk, stride=2), :] = im * sign

    def emit(kind, k):
        start, size = span(kind, k, 1 - b)
        blk = min(BLK, size)

        def body(i):
            s = start + i * blk
            re, im = load(bo, s, blk)
            if not kind:
                d = norm2((re, im))
                acc[rows(s % SR, blk), :] += d
                tot[s // SR] += fold(d)
            put(s, re, im, blk)
        loop(size // blk, body)

    sl = lax.broadcasted_iota(jnp.int32, (8, LANES), 0)
    ln = lax.broadcasted_iota(jnp.int32, (8, LANES), 1)

    def sgn(bit):
        return (1 - 2 * bit).astype(jnp.float32)

    def signed(terms, bit):
        parts = [-t if (v >> bit) & 1 else t for v, t in enumerate(terms)]
        while len(parts) > 1:
            parts = [parts[v] + parts[v + 1] for v in range(0, len(parts), 2)]
        return parts[0]

    def sums(half):
        units = [tot[half * NS + v] for v in range(NS)]
        total = signed([t for t in units], 30)
        wide = [acc[8 * v:8 * v + 8, :] for v in range(SR // 8)]
        vecs = [diff[0] * sgn(b), diff[1] * -sgn(b)] if half else [total * sgn(b), total * sgn(z % 2)]
        vecs += [total * sgn(my_bit(4 - q)) for q in range(2, 5)]
        vecs.append(-total if half else total)
        vecs += [signed(units, 10 - q) for q in range(6, 11)]
        vecs += [signed(wide, 14 - q) for q in range(11, 15)]
        vecs += [total * sgn((sl >> (17 - q)) & 1) for q in range(15, 18)]
        vecs += [total * sgn((ln >> (24 - q)) & 1) for q in range(18, 25)]
        parts = [jnp.sum(v, axis=0, keepdims=True) for v in vecs]
        return jnp.concatenate(parts + [jnp.zeros((1, LANES), jnp.float32)] * (32 - NQ), axis=0)

    acc[...] = jnp.zeros_like(acc)
    tot[...] = jnp.zeros_like(tot)
    loop(8, lambda k: emit(0, k))
    fvec[...] = sums(0)
    up_sums = remote(fvec, gvec, vs, vr, dev_in)

    @pl.when(outer)
    def _():
        up_sums.start()

    @pl.when(inner)
    def _():
        up_sums.wait_recv()
        fvec[...] += gvec[...]
        acc[...] = jnp.zeros_like(acc)
        diff[...] = jnp.zeros_like(diff)

    def phase5(k):
        finish_z(1, k)
        emit(1, k)
    loop(6, phase5)
    for k in range(NT - 1):
        finish_z(2, k, 4)
        emit(2, k)
    finish_z(2, NT - 1, 4)

    mine = b * 8 + sub

    def msg_copy(r):
        return remote(msg.at[mine], msg.at[mine], ms, mr, (me + r) % 32)

    @pl.when(inner)
    def _():
        wide = jnp.concatenate([fvec[...] + sums(1), jnp.zeros((LANES - 32, LANES), jnp.float32)], axis=0)
        msg[pl.ds(mine, 1)] = jnp.sum(wide.T, axis=0, keepdims=True)[None]
        loop(31, lambda r: msg_copy(r + 1).start())
        loop(ND - 1, lambda k: mid_copy(k + 1).start())
    emit(2, NT - 1)

    @pl.when(outer)
    def _():
        early_copy.wait_recv()
    w_near = [tuple(jnp.where(inner, p, q) for p, q in zip(*pair)) for pair in zip(w_own, (w_out[1], w_out[0]))]

    def take(k):
        mid_copy(k).wait_recv()

        def add_up(i):
            t = k * DP + i * BLK
            s = direct(1 - b) + t
            re, im = cmac(tuple(zip(w_near, (load(psi, s, BLK), load(abuf, s, BLK)))))
            far = load(rp, t, BLK)
            put(s, re + far[0], im + far[1], BLK)
        loop(DP // BLK, add_up)
    loop(ND, take)

    def receive(count):
        got = msg.at[pl.ds(0, count)]
        remote(got, got, ms, mr, dev_mid).wait_recv()

    @pl.when(inner)
    def _():
        receive(15)

    @pl.when(outer)
    def _():
        receive(16)
    val = msg[0]
    for t in range(1, 16):
        val = val + msg[t]
    z_ref[...] = (val * (1.0 / (ROWS * LANES * 32)))[:, :NQ]

    @pl.when(inner)
    def _():
        remote(abuf, bf, fs, vr, dev_mid).wait_send()
        remote(sent, sent, ms, vr, dev_mid).wait_send()
        remote(bf, bo, os_, vr, dev_out).wait_send()

    @pl.when(outer)
    def _():
        up_sums.wait_send()
    remote(psi, bo, ps, vr, dev_mid).wait_send()


def writer(s_ref, z_ref, o_hbm, zo_ref, sem):
    copies = [pltpu.make_async_copy(s_ref.at[pl.ds(k * 2 * ROWS // NW, 2 * ROWS // NW), :],
                                    o_hbm.at[pl.ds(k * 2 * ROWS // NW, 2 * ROWS // NW), :], sem.at[k]) for k in range(NW)]
    copies.append(pltpu.make_async_copy(z_ref, zo_ref, sem.at[NW]))
    for cp in copies:
        cp.start()
    for cp in copies:
        cp.wait()


def solution(mesh):
    dma = pltpu.SemaphoreType.DMA
    big = pltpu.VMEM((2, ROWS, LANES), jnp.float32)
    slots = pltpu.VMEM((2, NX * GR, LANES), jnp.float32)

    def local_layer(state_local, unitaries, cz_pairs):
        x = state_local.reshape(2, ROWS, LANES).transpose(1, 0, 2).reshape(2 * ROWS, LANES)
        gates = unitaries.transpose(0, 2, 3, 1)
        out, z_exp = pl.pallas_call(
            kernel,
            name="gate_layer",
            out_shape=(pltpu.VMEM((2 * ROWS, LANES), jnp.float32), pltpu.VMEM((1, NQ), jnp.float32)),
            in_specs=[pl.BlockSpec(memory_space=pl.ANY),
                      pl.BlockSpec(memory_space=pl.ANY),
                      pl.BlockSpec(memory_space=pl.ANY)],
            out_specs=(pl.BlockSpec(memory_space=pltpu.VMEM), pl.BlockSpec(memory_space=pltpu.VMEM)),
            scratch_shapes=[big] * 4 + [slots] * 3 + [
                pltpu.VMEM((4 * 2 * GR, LANES), jnp.float32),
                pltpu.VMEM((256, 256), jnp.float32),
                pltpu.VMEM((256, 256), jnp.float32),
                pltpu.VMEM((SR, LANES), jnp.float32),
                pltpu.VMEM((2 * NS, 8, LANES), jnp.float32),
                pltpu.VMEM((2, 8, LANES), jnp.float32),
                pltpu.VMEM((32, LANES), jnp.float32),
                pltpu.VMEM((32, LANES), jnp.float32),
                pltpu.VMEM((16, 1, LANES), jnp.float32),
                pltpu.VMEM((31, 1, LANES), jnp.float32),
                pltpu.VMEM((2, DR, LANES), jnp.float32),
                pltpu.VMEM((2, DR, LANES), jnp.float32),
                pltpu.VMEM((2, DR, LANES), jnp.float32),
                pltpu.SMEM((2, 2, 2, NQ), jnp.float32),
                pltpu.SMEM((2, 12), jnp.int32),
                dma((2,)), dma((4,)), dma(()), dma((NG,)), dma((NZ,)), dma(()), dma(())] + [
                dma((2,)), dma((NX,))] * 3 + [dma(())] * 5 + [dma((ND,))],
            compiler_params=pltpu.CompilerParams(has_side_effects=True, collective_id=0,
                                                 vmem_limit_bytes=VMEM_LIMIT),
        )(x, gates, cz_pairs.transpose(1, 0))
        out, z_exp = pl.pallas_call(
            writer,
            name="write_result",
            out_shape=(jax.ShapeDtypeStruct((2 * ROWS, LANES), jnp.float32), jax.ShapeDtypeStruct((1, NQ), jnp.float32)),
            in_specs=[pl.BlockSpec(memory_space=pltpu.VMEM), pl.BlockSpec(memory_space=pltpu.VMEM)],
            out_specs=(pl.BlockSpec(memory_space=pl.ANY), pl.BlockSpec(memory_space=pl.ANY)),
            scratch_shapes=[dma((NW + 1,))],
            compiler_params=pltpu.CompilerParams(vmem_limit_bytes=2 ** 20),
        )(out, z_exp)
        out = out.reshape(ROWS, 2, LANES).transpose(1, 0, 2).reshape(2, ROWS * LANES)
        return out, z_exp.reshape(NQ)

    return jax.shard_map(local_layer, mesh=mesh, in_specs=(P(None, 'q'), P(), P()),
                         out_specs=(P(None, 'q'), P()), check_vma=False)
```
